32 devices in a mesh: rows: 2 (over core), cols: 4 (over y, x), slabs: 4 (over z).
Axes of the slice: x: 2, y: 2, z: 4, core: 2. Of those that a mesh axis runs over, the one named last changes fastest.
Arguments:
- field_now: float32 [8, 128, 512, 128], P('rows', 'cols', 'slabs'), may hold values from 0.5 to 2
- earlier: float32 [8, 128, 512, 128], P('rows', 'cols', 'slabs'), may hold values from 0.2 to 1.8
- speed_square: float32 [8, 128, 512, 128], P('rows', 'cols', 'slabs'), may hold values from 0.05 to 0.3
Outputs:
- scaled_field: float32 [8, 128, 512, 128], P('rows', 'cols', 'slabs')
- field_now_end: float32 [8, 128, 512, 128], P('rows', 'cols', 'slabs')
The draws below stay inside these ranges and needn't reach their ends.
All inputs are finite; a program needn't handle non-finite values.
Results may differ from the reference program's by a relative error of at most 0.00002.
Values sent between devices are 32-bit elements; how exact they have to be, the bound alone decides.
A program may use at most 128 MiB of HBM per device.

```python
import jax
import jax.numpy as jnp
from jax import lax

GRID_J = 8
GRID_I = 128
GRID_K = 512
MEMBERS = 128
STEPS = 3


def block_levels(rng, shape, cuts, smallest, top_value):
    level, own = 1.0, jax.random.fold_in(rng, 6)
    for position, blocks in cuts:
        steps = jnp.exp(jax.random.uniform(jax.random.fold_in(own, position), (blocks,), jnp.float32, smallest / len(cuts), top_value / len(cuts)))
        level = level * jnp.repeat(steps, shape[position] // blocks).reshape([-1 if axis == position else 1 for axis in range(len(shape))])
    return level


def setup_inputs(seed: int = 0) -> dict:
    keys = jax.random.split(jax.random.key(seed), 4)
    field_now = jnp.clip(0.5 + 1.5 * jax.random.uniform(keys[0], (GRID_J, GRID_I, GRID_K, MEMBERS), jnp.float32) ** block_levels(keys[0], (GRID_J, GRID_I, GRID_K, MEMBERS), ((0, 2), (1, 4), (2, 4)), -0.2, 0.2), 0.5, 2.0)
    earlier = jnp.clip(0.2 + 1.5999999 * jax.random.uniform(keys[1], (GRID_J, GRID_I, GRID_K, MEMBERS), jnp.float32) ** block_levels(keys[1], (GRID_J, GRID_I, GRID_K, MEMBERS), ((0, 2), (1, 4), (2, 4)), -0.2, 0.2), 0.2, 1.8)
    speed_square = jnp.clip(0.05 + 0.25 * jax.random.uniform(keys[2], (GRID_J, GRID_I, GRID_K, MEMBERS), jnp.float32) ** block_levels(keys[2], (GRID_J, GRID_I, GRID_K, MEMBERS), ((0, 2), (1, 4), (2, 4)), -0.2, 0.2), 0.05, 0.3)
    return {"field_now": field_now, "earlier": earlier, "speed_square": speed_square}


def without_rim(values, dims):
    for dim in dims:
        values = lax.slice_in_dim(values, 1, values.shape[dim] - 1, axis=dim)
    return values

def shifted_cells(values, dim, start, dims):
    others = [other for other in dims if other != dim]
    values = without_rim(values, others)
    return lax.slice_in_dim(values, start, start + values.shape[dim] - 2, axis=dim)

def march_step(padded, before, speed_square):
    middle = without_rim(padded, (0, 1, 2))
    lower = [shifted_cells(padded, dim, 0, (0, 1, 2)) for dim in (0, 1, 2)]
    upper = [shifted_cells(padded, dim, 2, (0, 1, 2)) for dim in (0, 1, 2)]
    spread = lower[0] + upper[0] + lower[1] + upper[1] + lower[2] + upper[2] - 6.0 * middle
    return 2.0 * middle - before + speed_square * spread

def reference(field_now, earlier, speed_square):
    for step in range(STEPS):
        later = march_step(jnp.pad(field_now, ((1, 1), (1, 1), (1, 1), (0, 0)), mode='constant'), earlier, speed_square)
        earlier, field_now = (field_now, later)
    line_mean = lax.optimization_barrier(jnp.mean(field_now, axis=2, keepdims=True))
    centred = field_now - line_mean
    line_variance = lax.optimization_barrier(jnp.mean(centred * centred, axis=2, keepdims=True))
    scaled_field = centred * lax.rsqrt(line_variance + 0.0001)
    return (scaled_field, field_now)
```

```python
import functools

import jax
import jax.numpy as jnp
from jax import lax
from jax.experimental import pallas as pl
from jax.experimental.pallas import tpu as pltpu
from jax.sharding import PartitionSpec as P

STEPS = 3
EPS = 1e-4
MESH = pl.DeviceIdType.MESH
AXES = ("rows", "cols", "slabs")
OWN, DIAG = 0, 1


def line_parts(ni):
    return 4 if ni % 32 == 0 else 1


def edge_places(cols, ni):
    odd = lax.rem(cols, 2)
    return ni - odd * (ni - 1), 1 + odd * (ni - 1)


def march_kernel(
    counts, relay, now_hbm, old_hbm, speed_hbm, field, scaled, mean_ref, scale_ref,
    work, face_out, face_in, rim_out, rim_in, own_stats, own_edge, in_stats, all_edge, relayed,
    means, scales, load_x, load_y, load_c,
    side_send, side_recv, pass_send, pass_recv, row_send, row_recv, row_rim_send, row_rim_recv,
    slab_send, slab_recv, slab_rim_send, slab_rim_recv, stat_send, stat_recv, edge_send, edge_recv,
):
    nj, ni, nk, lanes = now_hbm.shape
    speed = scaled
    n_slabs = counts["slabs"]
    parts = line_parts(ni)
    width = ni // parts
    inside_out = [0, *range(parts - 1, 0, -1)] if parts > 1 else [0]
    outside_in = inside_out[2:] + inside_out[:2]
    here = {axis: lax.axis_index(axis) for axis in AXES}
    has_low = {axis: here[axis] > 0 for axis in AXES}
    has_high = {axis: here[axis] < counts[axis] - 1 for axis in AXES}
    odd = lax.rem(here["cols"], 2)
    places = edge_places(here["cols"], ni)
    beside = (here["cols"] + 1 - 2 * odd, here["cols"] - 1 + 2 * odd)
    has_side = tuple((other >= 0) & (other < counts["cols"]) for other in beside)
    halos = ((1 - odd) * (ni + 1), odd * (ni + 1))

    def span(part):
        return part * width, (part + 1) * width

    loads = {}
    for name, source in (("now", now_hbm), ("old", old_hbm), ("speed", speed_hbm)):
        for part in inside_out:
            start, _ = span(part)
            plain, padded = pl.ds(start, width), (pl.ds(1, nj), pl.ds(1 + start, width))
            target = {"now": work.at[padded], "old": field.at[padded], "speed": speed.at[:, plain]}[name]
            sem = {"now": load_x, "old": load_y, "speed": load_c}[name].at[part]
            loads[name, part] = pltpu.make_async_copy(source.at[:, plain], target, sem)
            loads[name, part].start()

    barrier = pltpu.get_barrier_semaphore()
    expected = jnp.int32(n_slabs - 1)
    for axis in ("rows", "cols"):
        for there, shift in ((has_low[axis], -1), (has_high[axis], 1)):
            expected = expected + there.astype(jnp.int32)

            @pl.when(there)
            def _():
                pl.semaphore_signal(barrier, inc=1, device_id={axis: here[axis] + shift}, device_id_type=MESH)

    peers = [lax.rem(here["slabs"] + gap, n_slabs) for gap in range(1, n_slabs)]
    for peer in peers:
        pl.semaphore_signal(barrier, inc=1, device_id={"slabs": peer}, device_id_type=MESH)
    if relay:
        over = lax.rem(here["cols"] + 2, 4)
        pl.semaphore_signal(barrier, inc=1, device_id={"cols": over}, device_id_type=MESH)
        expected = expected + 1
    pl.semaphore_wait(barrier, expected)

    half = nj // 2 if relay else 0
    relays = has_side[OWN] & ~has_side[DIAG]

    def buffer_of(step):
        return work if step % 2 == 0 else field

    def side_copy(step, which, j, kind="straight"):
        buffer = buffer_of(step)
        source = now_hbm.at[j, places[which] - 1] if step == 0 else buffer.at[j + 1, places[which]]
        target = beside[which]
        landing = buffer.at[j + 1, ni + 1 - halos[which]]
        sems = side_send.at[step, which, j], side_recv.at[step, which, j]
        if kind == "to":
            landing, target = relayed.at[step, j], over
            sems = sems[0], pass_recv.at[step, j]
        elif kind == "on":
            source, target = relayed.at[step, j], beside[OWN]
            landing = buffer.at[j + 1, halos[OWN]]
            sems = pass_send.at[step, j], sems[1]
        return pltpu.make_async_remote_copy(
            source, landing, *sems, device_id={"cols": target}, device_id_type=MESH
        )

    def side(step, which, j, what):
        relayed_line = which == DIAG and j < half
        if what == "start":
            pl.when(has_side[which])(side_copy(step, which, j, "to" if relayed_line else "straight").start)
        elif what == "sent":
            pl.when(has_side[which])(side_copy(step, which, j).wait_send)
        else:
            pl.when(has_side[which])(side_copy(step, which, j).wait_recv)

    def hand_on(step, j):
        if j < half:
            @pl.when(relays)
            def _():
                side_copy(step, DIAG, j, "to").wait_recv()
                side_copy(step, DIAG, j, "on").start()

    def run(copy, sends, takes, what):
        if what == "start":
            pl.when(sends)(copy.start)
        elif what == "sent":
            pl.when(sends)(copy.wait_send)
        else:
            pl.when(takes)(copy.wait_recv)

    def directions(axis):
        for to_high in (0, 1):
            sends = has_high[axis] if to_high else has_low[axis]
            takes = has_low[axis] if to_high else has_high[axis]
            yield to_high, sends, takes, here[axis] + (1 if to_high else -1)

    def segment(step, number):
        if number < parts:
            start, stop = span(number)
            rim = 1 if step < 2 else 2
            return max(1 + start, 1 + rim), min(1 + stop, 1 + ni - rim)
        place = 2 if number == parts else ni - 1
        return place, place + 1

    def rows(step, number, what):
        start, stop = segment(step, number)
        lines, buffer = pl.ds(start, stop - start), buffer_of(step)
        for to_high, sends, takes, target in directions("rows"):
            j = nj - 1 if to_high else 0
            source = now_hbm.at[j, pl.ds(start - 1, stop - start)] if step == 0 else buffer.at[j + 1, lines]
            copy = pltpu.make_async_remote_copy(
                source, buffer.at[0 if to_high else nj + 1, lines],
                row_send.at[step, to_high, number], row_recv.at[step, to_high, number],
                device_id={"rows": target}, device_id_type=MESH,
            )
            run(copy, sends, takes, what)

    def row_rim(step, which, to_highs, what):
        buffer = buffer_of(step)
        for to_high, sends, takes, target in directions("rows"):
            if to_high not in to_highs:
                continue
            j = nj - 1 if to_high else 0
            source = now_hbm.at[j, places[which] - 1] if step == 0 else buffer.at[j + 1, places[which]]
            copy = pltpu.make_async_remote_copy(
                source, buffer.at[0 if to_high else nj + 1, places[which]],
                row_rim_send.at[step, to_high, which], row_rim_recv.at[step, to_high, which],
                device_id={"rows": target}, device_id_type=MESH,
            )
            run(copy, sends, takes, what)

    def slabs(step, number, what):
        start, stop = segment(step, number)
        lines = pl.ds(start - 1, stop - start)
        for to_high, sends, takes, target in directions("slabs"):
            copy = pltpu.make_async_remote_copy(
                face_out.at[step, to_high, lines], face_in.at[step, to_high, lines],
                slab_send.at[step, to_high, number], slab_recv.at[step, to_high, number],
                device_id={"slabs": target}, device_id_type=MESH,
            )
            run(copy, sends, takes, what)

    def slab_rim(step, which, what):
        for to_high, sends, takes, target in directions("slabs"):
            copy = pltpu.make_async_remote_copy(
                rim_out.at[step, to_high, which], rim_in.at[step, to_high, which],
                slab_rim_send.at[step, to_high, which], slab_rim_recv.at[step, to_high, which],
                device_id={"slabs": target}, device_id_type=MESH,
            )
            run(copy, sends, takes, what)

    for j in range(half):
        side(0, DIAG, j, "start")
    for j in range(nj):
        side(0, OWN, j, "start")
    for j in range(half, nj):
        side(0, DIAG, j, "start")
    for which in (OWN, DIAG):
        row_rim(0, which, (0, 1), "start")
    for part in inside_out:
        rows(0, part, "start")

    zeros_line = jnp.zeros((nk, lanes), jnp.float32)
    for buffer in (work, field):
        for absent, edge in ((~has_low["rows"], 0), (~has_high["rows"], nj + 1)):
            @pl.when(absent)
            def _():
                @pl.loop(1, ni + 1)
                def _(i):
                    buffer[edge, i] = zeros_line
        for absent, edge in ((~has_low["cols"], 0), (~has_high["cols"], ni + 1)):
            @pl.when(absent)
            def _():
                @pl.loop(1, nj + 1)
                def _(j):
                    buffer[j, edge] = zeros_line
    for absent, to_high in ((~has_low["slabs"], 1), (~has_high["slabs"], 0)):
        @pl.when(absent)
        def _():
            for step in range(STEPS):
                face_in[step, to_high] = jnp.zeros((ni, nj, lanes), jnp.float32)
                rim_in[step, to_high] = jnp.zeros((2, nj, lanes), jnp.float32)
    own_stats[...] = jnp.zeros_like(own_stats)

    for part in inside_out:
        loads["now", part].wait()
        if part == inside_out[min(1, parts - 1)]:
            for which in (OWN, DIAG):
                for j in range(nj):
                    rim_out[0, 0, which, pl.ds(j, 1), :] = work[j + 1, places[which], pl.ds(0, 1), :]
                    rim_out[0, 1, which, pl.ds(j, 1), :] = work[j + 1, places[which], pl.ds(nk - 1, 1), :]
            for which in (OWN, DIAG):
                slab_rim(0, which, "start")
        start, stop = segment(0, part)

        @pl.loop(start, stop)
        def _(i):
            for j in range(nj):
                face_out[0, 0, i - 1, pl.ds(j, 1), :] = work[j + 1, i, pl.ds(0, 1), :]
                face_out[0, 1, i - 1, pl.ds(j, 1), :] = work[j + 1, i, pl.ds(nk - 1, 1), :]

        slabs(0, part, "start")

    groups = nk // 8
    row_number = lax.broadcasted_iota(jnp.int32, (8, lanes), 0)

    def line(step, i, js, rim=None):
        now, old = (work, field) if step % 2 == 1 else (field, work)
        last = step == STEPS
        sums = {}

        def halo(to_high, j):
            if rim is None:
                return face_in[step - 1, to_high, i - 1, pl.ds(j, 1), :]
            return rim_in[step - 1, to_high, rim, pl.ds(j, 1), :]

        def keep(to_high, j, row):
            if rim is None:
                face_out[step, to_high, i - 1, pl.ds(j, 1), :] = row
            else:
                rim_out[step, to_high, rim, pl.ds(j, 1), :] = row

        for g in range(groups):
            k = pl.ds(8 * g, 8)
            column = {j: now[j, i, k, :] for j in range(js[0], js[-1] + 3)}
            for j in js:
                middle = column[j + 1]
                if g == 0:
                    low = jnp.where(
                        row_number == 0, jnp.broadcast_to(halo(1, j), (8, lanes)), pltpu.roll(middle, 1, 0)
                    )
                else:
                    low = now[j + 1, i, pl.ds(8 * g - 1, 8), :]
                if g == groups - 1:
                    high = jnp.where(
                        row_number == 7, jnp.broadcast_to(halo(0, j), (8, lanes)), pltpu.roll(middle, 7, 0)
                    )
                else:
                    high = now[j + 1, i, pl.ds(8 * g + 1, 8), :]
                spread = (
                    (column[j] + column[j + 2])
                    + (now[j + 1, i - 1, k, :] + now[j + 1, i + 1, k, :])
                    + (low + high)
                    - 6.0 * middle
                )
                later = 2.0 * middle - old[j + 1, i, k, :] + speed[j, i - 1, k, :] * spread
                old[j + 1, i, k, :] = later
                if last:
                    sums[j] = later if g == 0 else sums[j] + later
                else:
                    if g == 0:
                        keep(0, j, later[0:1])
                    if g == groups - 1:
                        keep(1, j, later[7:8])
        if last:
            for j in js:
                total = jnp.sum(sums[j], axis=0, keepdims=True)
                mean = jnp.broadcast_to(total * (1.0 / nk), (8, lanes))
                squares = None
                for g in range(groups):
                    moved = old[j + 1, i, pl.ds(8 * g, 8), :] - mean
                    squares = moved * moved if g == 0 else squares + moved * moved
                square = jnp.sum(squares, axis=0, keepdims=True)
                if rim is None:
                    own_stats[0, 0, j, pl.ds(i - 1, 1), :] = total
                    own_stats[0, 1, j, pl.ds(i - 1, 1), :] = square
                else:
                    own_edge[0, pl.ds(rim * nj + j, 1), :] = total
                    own_edge[1, pl.ds(rim * nj + j, 1), :] = square

    every_j = tuple(range(nj))

    def interior(step, part):
        start, stop = span(part)
        rim = max(step, 1)
        start, stop = max(1 + start, 1 + rim), min(1 + stop, 1 + ni - rim)
        if step == 1:
            loads["old", part].wait()
            loads["speed", part].wait()
        rows(step - 1, part, "taken")
        slabs(step - 1, part, "taken")
        if step == 3:
            rows(1, part, "sent")

        @pl.loop(start, stop)
        def _(i):
            line(step, i, every_j)

        if step < STEPS:
            rows(step, part, "start")
            slabs(step, part, "start")

    def strips(step):
        if step == 2:
            for number, place in ((parts, 2), (parts + 1, ni - 1)):
                line(step, place, every_j)
                rows(step, number, "start")
                slabs(step, number, "start")
        else:
            for number in (parts, parts + 1):
                rows(step - 1, number, "taken")
                slabs(step - 1, number, "taken")
            for place in (3, ni - 2, 2, ni - 1):
                line(step, place, every_j)

    def edge(step, which, j):
        side(step - 1, which, j, "taken")
        order = edge_order[which]
        if j == order[0]:
            slab_rim(step - 1, which, "taken")
            if step == 3:
                row_rim(1, which, (0, 1), "sent")
        if j == 0:
            row_rim(step - 1, which, (1,), "taken")
        if j == nj - 1:
            row_rim(step - 1, which, (0,), "taken")
        if step == 3:
            side(1, which, j, "sent")
        line(step, places[which], (j,), which)
        if step < STEPS:
            side(step, which, j, "start")
            if j == 0:
                row_rim(step, which, (0,), "start")
            if j == nj - 1:
                row_rim(step, which, (1,), "start")
            if j == order[-1]:
                slab_rim(step, which, "start")

    edge_order = (
        list(range(nj)),
        [j for pair in zip(range(half), range(half, nj)) for j in pair] + list(range(2 * half, nj))
        if half else list(range(nj)),
    )

    levels = n_slabs.bit_length() - 1
    partners = []
    for level in range(levels):
        bit = lax.rem(here["slabs"] // 2**level, 2)
        partners.append(here["slabs"] + (1 - 2 * bit) * 2**level)

    def stat_copy(part, level):
        lines = pl.ds(part * width, width)
        return pltpu.make_async_remote_copy(
            own_stats.at[level, :, :, lines], in_stats.at[level, :, :, lines],
            stat_send.at[part, level], stat_recv.at[part, level],
            device_id={"slabs": partners[level]}, device_id_type=MESH,
        )

    def edge_copy(gap):
        return pltpu.make_async_remote_copy(
            own_edge, all_edge.at[gap - 1], edge_send.at[gap - 1], edge_recv.at[gap - 1],
            device_id={"slabs": peers[gap - 1]}, device_id_type=MESH,
        )

    def merged(part, level):
        lines = pl.ds(part * width, width)
        stat_copy(part, level).wait_recv()
        mine, theirs = own_stats[level, :, :, lines, :], in_stats[level, :, :, lines, :]
        cells = float(nk * 2**level)
        apart = (theirs[0] - mine[0]) * (1.0 / cells)
        return mine[0] + theirs[0], mine[1] + theirs[1] + (0.5 * cells) * apart * apart

    def advance(part, level):
        lines = pl.ds(part * width, width)
        total, square = merged(part, level)
        own_stats[level + 1, 0, :, lines, :] = total
        own_stats[level + 1, 1, :, lines, :] = square
        stat_copy(part, level + 1).start()

    whole = float(nk * n_slabs)

    def rescale(part):
        lines = pl.ds(part * width, width)
        total, square = merged(part, levels - 1)
        means[:, lines, :] = total * (1.0 / whole)
        scales[:, lines, :] = lax.rsqrt(square * (1.0 / whole) + EPS)
        start, stop = span(part)

        @pl.loop(max(start, 1), min(stop, ni - 1))
        def _(i):
            for j in range(nj):
                mean = jnp.broadcast_to(means[j, pl.ds(i, 1), :], (8, lanes))
                scale = jnp.broadcast_to(scales[j, pl.ds(i, 1), :], (8, lanes))
                for g in range(groups):
                    k = pl.ds(8 * g, 8)
                    scaled[j, i, k, :] = (field[j + 1, i + 1, k, :] - mean) * scale

    def do(kind, *what):
        if kind == "in":
            interior(what[0], what[1])
        elif kind == "own":
            edge(what[0], OWN, edge_order[OWN][what[1]])
        elif kind == "diag":
            edge(what[0], DIAG, edge_order[DIAG][what[1]])
        elif kind == "pass":
            hand_on(*what)
        elif kind == "strips":
            strips(what[0])
        elif kind == "stats":
            stat_copy(what[0], 0).start()
        elif kind == "advance":
            for level in range(levels - 1):
                advance(what[0], level)
        elif kind == "rescale":
            rescale(what[0])

    for what in agenda(nj, parts, inside_out, outside_in):
        do(*what)

    gaps = range(1, n_slabs)
    for gap in gaps:
        edge_copy(gap).start()
    for part in outside_in:
        rescale(part)

    def combine(own, others):
        mean = own[0]
        for other in others:
            mean = mean + other[0]
        mean = mean * (1.0 / whole)
        square = None
        for one in (own, *others):
            gap = one[0] * (1.0 / nk) - mean
            term = one[1] + nk * gap * gap
            square = term if square is None else square + term
        return mean, lax.rsqrt(square * (1.0 / whole) + EPS)

    for step in range(STEPS):
        for which in (OWN, DIAG):
            for j in range(nj):
                if step != 1:
                    side(step, which, j, "sent")
            if step != 1:
                row_rim(step, which, (0, 1), "sent")
            slab_rim(step, which, "sent")
        for j in range(half):
            pl.when(relays)(side_copy(step, DIAG, j, "on").wait_send)
        for number in range(parts + 2 if step == 2 else parts):
            if step != 1:
                rows(step, number, "sent")
            slabs(step, number, "sent")
    for part in range(parts):
        for level in range(levels):
            stat_copy(part, level).wait_send()
    for gap in gaps:
        edge_copy(gap).wait_recv()
    mean, scale = combine(own_edge[...], [all_edge[gap - 1] for gap in gaps])
    mean_ref[...] = mean
    scale_ref[...] = scale
    for gap in gaps:
        edge_copy(gap).wait_send()


def agenda(nj, parts, first, last):
    passes = [[("pass", step, j) for j in range(nj)] for step in range(STEPS)]
    own = {step: [("own", step, n) for n in range(nj)] for step in range(1, STEPS + 1)}
    diag = {step: [("diag", step, n) for n in range(nj)] for step in range(1, STEPS + 1)}
    fill = {step: [("in", step, part) for part in (last if step == 3 else first)] for step in (1, 2, 3)}
    order = []

    def put(*lists):
        for some in lists:
            order.extend(some)

    def weave(*lists):
        spots = [((n + 0.5) / len(some), number, entry) for number, some in enumerate(lists) for n, entry in enumerate(some)]
        order.extend(entry for _, _, entry in sorted(spots, key=lambda spot: spot[:2]))

    two = max(parts // 2, 1)
    half = nj // 2
    put(fill[1][:1])
    weave(fill[1][1:], [entry for n in range(nj) for entry in (passes[0][n], own[1][n])])
    weave(diag[1], fill[2][:two])
    put([("strips", 2)])
    weave([entry for n in range(nj) for entry in (passes[1][n], own[2][n])], fill[2][two:] + fill[3][:1])
    weave(diag[2], fill[3][1:two + 1])
    put(fill[3][two + 1:])
    put([("strips", 3)])
    stats = [("stats", part) for part in last]
    put(stats)
    weave([entry for n in range(nj) for entry in (passes[2][n], own[3][n])], [("advance", part) for part in last])
    put(diag[3])
    return order


def finish_kernel(field, scaled, mean_ref, scale_ref, scaled_hbm, field_hbm, rims, field_sem, scaled_sem, rim_sem):
    nj, ni, nk, lanes = scaled_hbm.shape
    copies = []
    for j in range(nj):
        copies.append(pltpu.make_async_copy(field.at[j + 1, pl.ds(1, ni)], field_hbm.at[j], field_sem.at[j]))
        inner = pl.ds(1, ni - 2)
        copies.append(pltpu.make_async_copy(scaled.at[j, inner], scaled_hbm.at[j, inner], scaled_sem.at[j]))
    for copy in copies:
        copy.start()
    places = edge_places(lax.axis_index("cols"), ni)
    for which in (OWN, DIAG):
        for j in range(nj):
            row = pl.ds(which * nj + j, 1)
            mean = jnp.broadcast_to(mean_ref[row, :], (8, lanes))
            scale = jnp.broadcast_to(scale_ref[row, :], (8, lanes))
            for g in range(nk // 8):
                k = pl.ds(8 * g, 8)
                rims[which, j, k, :] = (field[j + 1, places[which], k, :] - mean) * scale
        copy = pltpu.make_async_copy(rims.at[which], scaled_hbm.at[:, places[which] - 1], rim_sem.at[which])
        copy.start()
        copies.append(copy)
    for copy in copies:
        copy.wait()


def shards(counts, relay, field_now, earlier, speed_square):
    nj, ni, nk, lanes = field_now.shape
    n_slabs = counts["slabs"]
    levels = n_slabs.bit_length() - 1
    assert n_slabs == 2**levels and levels >= 1
    relay = relay and nj > 1
    parts = line_parts(ni)
    f32 = jnp.float32
    padded = (nj + 2, ni + 2, nk, lanes)
    hbm = pl.BlockSpec(memory_space=pltpu.HBM)
    vmem = pl.BlockSpec(memory_space=pltpu.VMEM)
    cells = nj * ni * nk * lanes
    dma = pltpu.SemaphoreType.DMA
    field, scaled, mean, scale = pl.pallas_call(
        functools.partial(march_kernel, counts, relay),
        name="march",
        out_shape=(
            pltpu.VMEM(padded, f32),
            pltpu.VMEM((nj, ni, nk, lanes), f32),
            pltpu.VMEM((2 * nj, lanes), f32),
            pltpu.VMEM((2 * nj, lanes), f32),
        ),
        in_specs=[hbm] * 3,
        out_specs=(vmem,) * 4,
        scratch_shapes=[
            pltpu.VMEM(padded, f32),
            pltpu.VMEM((STEPS, 2, ni, nj, lanes), f32),
            pltpu.VMEM((STEPS, 2, ni, nj, lanes), f32),
            pltpu.VMEM((STEPS, 2, 2, nj, lanes), f32),
            pltpu.VMEM((STEPS, 2, 2, nj, lanes), f32),
            pltpu.VMEM((levels, 2, nj, ni, lanes), f32),
            pltpu.VMEM((2, 2 * nj, lanes), f32),
            pltpu.VMEM((levels, 2, nj, ni, lanes), f32),
            pltpu.VMEM((n_slabs - 1, 2, 2 * nj, lanes), f32),
            pltpu.VMEM((STEPS, max(nj // 2, 1), nk, lanes), f32),
            pltpu.VMEM((nj, ni, lanes), f32),
            pltpu.VMEM((nj, ni, lanes), f32),
            dma((parts,)),
            dma((parts,)),
            dma((parts,)),
            dma((STEPS, 2, nj)),
            dma((STEPS, 2, nj)),
            dma((STEPS, max(nj // 2, 1))),
            dma((STEPS, max(nj // 2, 1))),
            dma((STEPS, 2, parts + 2)),
            dma((STEPS, 2, parts + 2)),
            dma((STEPS, 2, 2)),
            dma((STEPS, 2, 2)),
            dma((STEPS, 2, parts + 2)),
            dma((STEPS, 2, parts + 2)),
            dma((STEPS, 2, 2)),
            dma((STEPS, 2, 2)),
            dma((parts, levels)),
            dma((parts, levels)),
            dma((n_slabs - 1,)),
            dma((n_slabs - 1,)),
        ],
        compiler_params=pltpu.CompilerParams(
            collective_id=0, has_side_effects=True, vmem_limit_bytes=40 * 2**20
        ),
        cost_estimate=pl.CostEstimate(flops=33 * cells, bytes_accessed=12 * cells, transcendentals=0),
    )(field_now, earlier, speed_square)
    return pl.pallas_call(
        finish_kernel,
        name="finish",
        out_shape=(jax.ShapeDtypeStruct(field_now.shape, f32),) * 2,
        in_specs=[vmem] * 4,
        out_specs=(hbm,) * 2,
        scratch_shapes=[
            pltpu.VMEM((2, nj, nk, lanes), f32),
            dma((nj,)),
            dma((nj,)),
            dma((2,)),
        ],
        compiler_params=pltpu.CompilerParams(vmem_limit_bytes=16 * 2**20),
        cost_estimate=pl.CostEstimate(flops=2 * cells, bytes_accessed=8 * cells, transcendentals=0),
    )(field, scaled, mean, scale)


def crosses(mesh):
    order = ("rows", "cols", "slabs")
    devices = mesh.devices.transpose([mesh.axis_names.index(axis) for axis in order])
    if devices.shape[1] != 4:
        return False
    one, other = (getattr(devices[0, place, 0], "coords", None) for place in (1, 2))
    return one is not None and sum(a != b for a, b in zip(one, other)) > 1


def solution(mesh):
    spec = P("rows", "cols", "slabs", None)
    return jax.shard_map(
        functools.partial(shards, dict(mesh.shape), crosses(mesh)),
        mesh=mesh,
        in_specs=(spec,) * 3,
        out_specs=(spec,) * 2,
        check_vma=False,
    )
```

```python
import functools

import jax
import jax.numpy as jnp
from jax import lax
from jax.experimental import pallas as pl
from jax.experimental.pallas import tpu as pltpu
from jax.sharding import PartitionSpec as P

STEPS = 3
EPS = 1e-4
MESH = pl.DeviceIdType.MESH
AXES = ("rows", "cols", "slabs")
OWN, DIAG = 0, 1
FILL = ((6.7, 7.7, 8.9, 9.8), (10.6, 11.8, 12.6, 13.6), (15.6, 16.4, 17.7, 19.2))
PASS = ((7.2, 8.6), (15.3, 18.9), (24.5, 27.4))
EDGE = (
    ((8.65, 8.7, 11.4, 15.4), (11.7, 14.6, 11.5, 14.1)),
    ((16.3, 17.6, 19.1, 24.6), (20.6, 23.5, 21.4, 24.3)),
    ((25.0, 26.5, 28.0, 32.0), (29.5, 32.5, 30.3, 31.8)),
)
STRIPS = (15.5, 24.7)
STATS = (20.5, 24.8)
ADVANCE = (25.3, 28.2)


def line_parts(ni):
    return 4 if ni % 32 == 0 else 1


def edge_places(cols, ni):
    odd = lax.rem(cols, 2)
    return ni - odd * (ni - 1), 1 + odd * (ni - 1)


def march_kernel(
    counts, relay, now_hbm, old_hbm, speed_hbm, field, scaled, mean_ref, scale_ref,
    work, face_out, face_in, rim_out, rim_in, own_stats, own_edge, in_stats, all_edge, relayed,
    means, scales, load_x, load_y, load_c,
    side_send, side_recv, pass_send, pass_recv, row_send, row_recv, row_rim_send, row_rim_recv,
    slab_send, slab_recv, slab_rim_send, slab_rim_recv, stat_send, stat_recv, edge_send, edge_recv,
):
    nj, ni, nk, lanes = now_hbm.shape
    speed = scaled
    n_slabs = counts["slabs"]
    parts = line_parts(ni)
    width = ni // parts
    inside_out = [0, *range(parts - 1, 0, -1)]
    outside_in = inside_out[2:] + inside_out[:2]
    here = {axis: lax.axis_index(axis) for axis in AXES}
    has_low = {axis: here[axis] > 0 for axis in AXES}
    has_high = {axis: here[axis] < counts[axis] - 1 for axis in AXES}
    odd = lax.rem(here["cols"], 2)
    places = edge_places(here["cols"], ni)
    beside = (here["cols"] + 1 - 2 * odd, here["cols"] - 1 + 2 * odd)
    has_side = tuple((other >= 0) & (other < counts["cols"]) for other in beside)
    halos = ((1 - odd) * (ni + 1), odd * (ni + 1))

    def span(part):
        return part * width, (part + 1) * width

    def load(name, part):
        start, _ = span(part)
        plain, padded = pl.ds(start, width), (pl.ds(1, nj), pl.ds(1 + start, width))
        source, target, sem = {
            "now": (now_hbm, work.at[padded], load_x),
            "old": (old_hbm, field.at[padded], load_y),
            "speed": (speed_hbm, speed.at[:, plain], load_c),
        }[name]
        return pltpu.make_async_copy(source.at[:, plain], target, sem.at[part])

    for part in inside_out:
        load("now", part).start()
    for part in inside_out[:2]:
        load("old", part).start()
        load("speed", part).start()

    barrier = pltpu.get_barrier_semaphore()
    expected = jnp.int32(0)
    for axis in AXES:
        for there, shift in ((has_low[axis], -1), (has_high[axis], 1)):
            expected = expected + there.astype(jnp.int32)

            @pl.when(there)
            def _():
                pl.semaphore_signal(barrier, inc=1, device_id={axis: here[axis] + shift}, device_id_type=MESH)

    peers = [lax.rem(here["slabs"] + gap, n_slabs) for gap in range(1, n_slabs)]
    if relay:
        over = lax.rem(here["cols"] + 2, 4)
        pl.semaphore_signal(barrier, inc=1, device_id={"cols": over}, device_id_type=MESH)
        expected = expected + 1
    pl.semaphore_wait(barrier, expected)
    for part in inside_out[2:]:
        load("old", part).start()
        load("speed", part).start()

    half = nj // 2 if relay else 0
    relays = has_side[OWN] & ~has_side[DIAG]

    def buffer_of(step):
        return work if step % 2 == 0 else field

    def remote(source, landing, send, recv, axis, target):
        return pltpu.make_async_remote_copy(
            source, landing, send, recv, device_id={axis: target}, device_id_type=MESH
        )

    def directions(axis):
        for to_high in (0, 1):
            yield to_high, has_high[axis] if to_high else has_low[axis], here[axis] + (1 if to_high else -1)

    def taken(axis, one, two):
        pl.when(has_low[axis] & has_high[axis])(two.wait_recv)
        pl.when(has_low[axis] ^ has_high[axis])(one.wait_recv)

    def side_copy(step, which, j, kind="straight"):
        buffer = buffer_of(step)
        source, target = buffer.at[j + 1, places[which]], beside[which]
        landing = buffer.at[j + 1, ni + 1 - halos[which]]
        sems = side_send.at[step % 2, which], side_recv.at[step % 2, which, j]
        if kind == "to":
            landing, target = relayed.at[step, j], over
            sems = sems[0], pass_recv.at[step % 2, j]
        elif kind == "on":
            source, landing, target = relayed.at[step, j], buffer.at[j + 1, halos[OWN]], beside[OWN]
            sems = pass_send, sems[1]
        return remote(source, landing, *sems, "cols", target)

    def side(step, which, j, what):
        relayed_line = which == DIAG and j < half
        if what == "start":
            pl.when(has_side[which])(side_copy(step, which, j, "to" if relayed_line else "straight").start)
        else:
            pl.when(has_side[which])(side_copy(step, which, j).wait_recv)

    def side_sent(step, which):
        lines = buffer_of(step).at[pl.ds(1, nj), places[which]]
        copy = remote(lines, lines, side_send.at[step % 2, which], side_recv.at[step % 2, which, 0], "cols", beside[which])
        pl.when(has_side[which])(copy.wait_send)

    def hand_on(step, j):
        @pl.when(relays)
        def _():
            side_copy(step, DIAG, j, "to").wait_recv()
            side_copy(step, DIAG, j, "on").start()

    def segment(step, number):
        if number < parts:
            start, stop = span(number)
            rim = 1 if step < 2 else 2
            return max(1 + start, 1 + rim), min(1 + stop, 1 + ni - rim)
        place = 2 if number == parts else ni - 1
        return place, place + 1

    def slot(step, number):
        return step % 2 * parts + number if number < parts else parts + number

    def rows(step, number, what):
        start, stop = segment(step, number)
        lines, buffer, recv = pl.ds(start, stop - start), buffer_of(step), row_recv.at[slot(step, number)]
        if what == "taken":
            one, two = (buffer.at[pl.ds(0, n), lines] for n in (1, 2))
            send = row_send.at[step % 2, 0]
            taken("rows", *(remote(some, some, send, recv, "rows", here["rows"]) for some in (one, two)))
            return
        for to_high, there, target in directions("rows"):
            source, landing = (nj, 0) if to_high else (1, nj + 1)
            copy = remote(
                buffer.at[source, lines], buffer.at[landing, lines], row_send.at[step % 2, to_high], recv, "rows", target
            )
            pl.when(there)(copy.start)

    def rows_sent(step):
        for to_high, there, target in directions("rows"):
            lines = buffer_of(step).at[nj if to_high else 1, pl.ds(2, ni - 2)]
            copy = remote(lines, lines, row_send.at[step % 2, to_high], row_recv.at[0], "rows", target)
            pl.when(there)(copy.wait_send)

    def row_rim(step, which, to_highs, what):
        buffer = buffer_of(step)
        for to_high, there, target in directions("rows"):
            if to_high not in to_highs:
                continue
            source, landing = (nj, 0) if to_high else (1, nj + 1)
            copy = remote(
                buffer.at[source, places[which]], buffer.at[landing, places[which]],
                row_rim_send.at[step % 2, to_high], row_rim_recv.at[step % 2, to_high, which], "rows", target,
            )
            if what == "start":
                pl.when(there)(copy.start)
            else:
                pl.when(has_low["rows"] if to_high else has_high["rows"])(copy.wait_recv)

    def row_rim_sent(step):
        for to_high, there, target in directions("rows"):
            lines = buffer_of(step).at[nj if to_high else 1, pl.ds(1, 2)]
            copy = remote(
                lines, lines, row_rim_send.at[step % 2, to_high], row_rim_recv.at[0, to_high, 0], "rows", target
            )
            pl.when(there)(copy.wait_send)

    def slabs(step, number, what):
        start, stop = segment(step, number)
        lines, recv = pl.ds(start - 1, stop - start), slab_recv.at[slot(step, number)]
        if what == "taken":
            one, two = (face_in.at[step, pl.ds(0, n), lines] for n in (1, 2))
            taken("slabs", *(remote(some, some, slab_send.at[0], recv, "slabs", here["slabs"]) for some in (one, two)))
            return
        for to_high, there, target in directions("slabs"):
            copy = remote(
                face_out.at[step, to_high, lines], face_in.at[step, to_high, lines],
                slab_send.at[to_high], recv, "slabs", target,
            )
            pl.when(there)(copy.start)

    def slab_rim(step, which, j, what):
        recv = slab_rim_recv.at[step % 2, which, j]
        if what == "taken":
            one, two = (rim_in.at[step, pl.ds(0, n), which, j] for n in (1, 2))
            taken("slabs", *(remote(some, some, slab_rim_send.at[0], recv, "slabs", here["slabs"]) for some in (one, two)))
            return
        for to_high, there, target in directions("slabs"):
            copy = remote(
                rim_out.at[step, to_high, which, j], rim_in.at[step, to_high, which, j],
                slab_rim_send.at[to_high], recv, "slabs", target,
            )
            pl.when(there)(copy.start)

    def slabs_sent():
        for to_high, there, target in directions("slabs"):
            faces, rims = face_out.at[:, to_high, pl.ds(1, ni - 2)], rim_out.at[:, to_high]
            pl.when(there)(remote(faces, faces, slab_send.at[to_high], slab_recv.at[0], "slabs", target).wait_send)
            copy = remote(rims, rims, slab_rim_send.at[to_high], slab_rim_recv.at[0, 0, 0], "slabs", target)
            pl.when(there)(copy.wait_send)

    for part in inside_out[:2]:
        load("now", part).wait()
    for j in range(half):
        side(0, DIAG, j, "start")
    first_sends, late_sends = opening(nj, half)
    for which, j in first_sends:
        side(0, which, j, "start")
    for which in (OWN, DIAG):
        for j in range(nj):
            rim_out[0, 0, which, j] = work[j + 1, places[which], pl.ds(0, 1), :]
            rim_out[0, 1, which, j] = work[j + 1, places[which], pl.ds(nk - 1, 1), :]
    for which in (OWN, DIAG):
        row_rim(0, which, (0, 1), "start")
        for j in range(nj):
            slab_rim(0, which, j, "start")

    zeros_line = jnp.zeros((nk, lanes), jnp.float32)
    for buffer in (work, field):
        for absent, edge in ((~has_low["rows"], 0), (~has_high["rows"], nj + 1)):
            @pl.when(absent)
            def _():
                @pl.loop(1, ni + 1)
                def _(i):
                    buffer[edge, i] = zeros_line
        for absent, edge in ((~has_low["cols"], 0), (~has_high["cols"], ni + 1)):
            @pl.when(absent)
            def _():
                @pl.loop(1, nj + 1)
                def _(j):
                    buffer[j, edge] = zeros_line
    for absent, to_high in ((~has_low["slabs"], 1), (~has_high["slabs"], 0)):
        @pl.when(absent)
        def _():
            for step in range(STEPS):
                face_in[step, to_high] = jnp.zeros((ni, nj, lanes), jnp.float32)
                rim_in[step, to_high] = jnp.zeros((2, nj, 1, lanes), jnp.float32)
    own_stats[...] = jnp.zeros_like(own_stats)

    for part in inside_out:
        if part not in inside_out[:2]:
            load("now", part).wait()
        rows(0, part, "start")
        start, stop = segment(0, part)

        @pl.loop(start, stop)
        def _(i):
            for j in range(nj):
                face_out[0, 0, i - 1, pl.ds(j, 1), :] = work[j + 1, i, pl.ds(0, 1), :]
                face_out[0, 1, i - 1, pl.ds(j, 1), :] = work[j + 1, i, pl.ds(nk - 1, 1), :]

        slabs(0, part, "start")

    groups = nk // 8
    row_number = lax.broadcasted_iota(jnp.int32, (8, lanes), 0)

    def line(step, i, js, rim=None):
        now, old = (work, field) if step % 2 == 1 else (field, work)
        last = step == STEPS
        sums = {}

        def halo(to_high, j):
            if rim is None:
                return face_in[step - 1, to_high, i - 1, pl.ds(j, 1), :]
            return rim_in[step - 1, to_high, rim, j]

        def keep(to_high, j, row):
            if rim is None:
                face_out[step, to_high, i - 1, pl.ds(j, 1), :] = row
            else:
                rim_out[step, to_high, rim, j] = row

        for g in range(groups):
            k = pl.ds(8 * g, 8)
            column = {j: now[j, i, k, :] for j in range(js[0], js[-1] + 3)}
            for j in js:
                middle = column[j + 1]
                if g == 0:
                    low = jnp.where(
                        row_number == 0, jnp.broadcast_to(halo(1, j), (8, lanes)), pltpu.roll(middle, 1, 0)
                    )
                else:
                    low = now[j + 1, i, pl.ds(8 * g - 1, 8), :]
                if g == groups - 1:
                    high = jnp.where(
                        row_number == 7, jnp.broadcast_to(halo(0, j), (8, lanes)), pltpu.roll(middle, 7, 0)
                    )
                else:
                    high = now[j + 1, i, pl.ds(8 * g + 1, 8), :]
                spread = (
                    (column[j] + column[j + 2])
                    + (now[j + 1, i - 1, k, :] + now[j + 1, i + 1, k, :])
                    + (low + high)
                    - 6.0 * middle
                )
                later = 2.0 * middle - old[j + 1, i, k, :] + speed[j, i - 1, k, :] * spread
                old[j + 1, i, k, :] = later
                if last:
                    sums[j] = later if g == 0 else sums[j] + later
                else:
                    if g == 0:
                        keep(0, j, later[0:1])
                    if g == groups - 1:
                        keep(1, j, later[7:8])
        if last:
            for j in js:
                total = jnp.sum(sums[j], axis=0, keepdims=True)
                mean = jnp.broadcast_to(total * (1.0 / nk), (8, lanes))
                squares = None
                for g in range(groups):
                    moved = old[j + 1, i, pl.ds(8 * g, 8), :] - mean
                    squares = moved * moved if g == 0 else squares + moved * moved
                square = jnp.sum(squares, axis=0, keepdims=True)
                if rim is None:
                    own_stats[0, 0, j, pl.ds(i - 1, 1), :] = total
                    own_stats[0, 1, j, pl.ds(i - 1, 1), :] = square
                else:
                    own_edge[0, pl.ds(rim * nj + j, 1), :] = total
                    own_edge[1, pl.ds(rim * nj + j, 1), :] = square

    every_j, begun = tuple(range(nj)), set()

    def interior(step, part):
        start, stop = span(part)
        rim = max(step, 1)
        start, stop = max(1 + start, 1 + rim), min(1 + stop, 1 + ni - rim)
        if step == 1:
            load("old", part).wait()
            load("speed", part).wait()
        rows(step - 1, part, "taken")
        slabs(step - 1, part, "taken")
        if step >= 2 and step not in begun:
            begun.add(step)
            rows_sent(step - 2)

        @pl.loop(start, stop)
        def _(i):
            line(step, i, every_j)

        if step < STEPS:
            rows(step, part, "start")
            slabs(step, part, "start")

    def strips(step):
        if step == 2:
            for number, place in ((parts, 2), (parts + 1, ni - 1)):
                line(step, place, every_j)
                rows(step, number, "start")
                slabs(step, number, "start")
        else:
            for number in (parts, parts + 1):
                rows(step - 1, number, "taken")
                slabs(step - 1, number, "taken")
            for place in (3, ni - 2, 2, ni - 1):
                line(step, place, every_j)

    def edge(step, which, j):
        side(step - 1, which, j, "taken")
        slab_rim(step - 1, which, j, "taken")
        shared = [to_high for to_high, place in ((0, 0), (1, nj - 1)) if place == j]
        row_rim(step - 1, which, [1 - to_high for to_high in shared], "taken")
        if step >= 2 and (step, which) not in begun:
            begun.add((step, which))
            side_sent(step - 2, which)
            if (step, OWN + DIAG - which) not in begun:
                row_rim_sent(step - 2)
        line(step, places[which], (j,), which)
        if step < STEPS:
            side(step, which, j, "start")
            slab_rim(step, which, j, "start")
            row_rim(step, which, shared, "start")

    levels = n_slabs.bit_length() - 1
    partners = []
    for level in range(levels):
        bit = lax.rem(here["slabs"] // 2**level, 2)
        partners.append(here["slabs"] + (1 - 2 * bit) * 2**level)

    def stat_copy(part, level):
        lines = pl.ds(part * width, width)
        return remote(
            own_stats.at[level, :, :, lines], in_stats.at[level, :, :, lines],
            stat_send, stat_recv.at[part, level], "slabs", partners[level],
        )

    def merged(part, level):
        lines = pl.ds(part * width, width)
        stat_copy(part, level).wait_recv()
        mine, theirs = own_stats[level, :, :, lines, :], in_stats[level, :, :, lines, :]
        cells = float(nk * 2**level)
        apart = (theirs[0] - mine[0]) * (1.0 / cells)
        return mine[0] + theirs[0], mine[1] + theirs[1] + (0.5 * cells) * apart * apart

    def advance(part, level):
        lines = pl.ds(part * width, width)
        total, square = merged(part, level)
        own_stats[level + 1, 0, :, lines, :] = total
        own_stats[level + 1, 1, :, lines, :] = square
        stat_copy(part, level + 1).start()

    whole = float(nk * n_slabs)

    def rescale(part):
        lines = pl.ds(part * width, width)
        total, square = merged(part, levels - 1)
        means[:, lines, :] = total * (1.0 / whole)
        scales[:, lines, :] = lax.rsqrt(square * (1.0 / whole) + EPS)
        start, stop = span(part)

        @pl.loop(max(start, 1), min(stop, ni - 1))
        def _(i):
            for j in range(nj):
                mean = jnp.broadcast_to(means[j, pl.ds(i, 1), :], (8, lanes))
                scale = jnp.broadcast_to(scales[j, pl.ds(i, 1), :], (8, lanes))
                for g in range(groups):
                    k = pl.ds(8 * g, 8)
                    scaled[j, i, k, :] = (field[j + 1, i + 1, k, :] - mean) * scale

    def do(kind, *what):
        if kind == "in":
            interior(what[0], what[1])
        elif kind == "own":
            edge(what[0], OWN, what[1])
        elif kind == "diag":
            edge(what[0], DIAG, what[1])
        elif kind == "pass":
            hand_on(*what)
        elif kind == "late":
            for which, j in late_sends:
                side(0, which, j, "start")
        elif kind == "strips":
            strips(what[0])
        elif kind == "stats":
            stat_copy(what[0], 0).start()
        elif kind == "advance":
            for level in range(levels - 1):
                advance(what[0], level)
        elif kind == "rescale":
            rescale(what[0])

    for what in agenda(nj, half, parts, inside_out, outside_in):
        do(*what)

    gaps = range(1, n_slabs)
    for gap in gaps:
        remote(own_edge, all_edge.at[gap - 1], edge_send, edge_recv, "slabs", peers[gap - 1]).start()
    for part in outside_in:
        rescale(part)

    def combine(own, others):
        mean = own[0]
        for other in others:
            mean = mean + other[0]
        mean = mean * (1.0 / whole)
        square = None
        for one in (own, *others):
            gap = one[0] * (1.0 / nk) - mean
            term = one[1] + nk * gap * gap
            square = term if square is None else square + term
        return mean, lax.rsqrt(square * (1.0 / whole) + EPS)

    for step in range(STEPS):
        if step == 2:
            for which in (OWN, DIAG):
                side_sent(step, which)
            row_rim_sent(step)
            rows_sent(step)
    slabs_sent()
    if half:
        pl.when(relays)(remote(relayed, relayed, pass_send, pass_recv.at[0, 0], "cols", beside[OWN]).wait_send)
    remote(own_stats, in_stats, stat_send, stat_recv.at[0, 0], "slabs", partners[0]).wait_send()
    edges = remote(all_edge, all_edge, edge_send, edge_recv, "slabs", peers[0])
    edges.wait_recv()
    mean, scale = combine(own_edge[...], [all_edge[gap - 1] for gap in gaps])
    mean_ref[...] = mean
    scale_ref[...] = scale
    edges.wait_send()


def opening(nj, half):
    own, diag = [(OWN, j) for j in range(nj)], [(DIAG, j) for j in range(half, nj)]
    woven = [(OWN, j) for j in range(nj - len(diag))]
    for late, line in zip(own[nj - len(diag):], diag):
        woven += [line, late]
    return woven[:-2], woven[-2:]


def agenda(nj, half, parts, first, last):
    timed = []

    def spread(times, entries):
        for n, entry in enumerate(entries):
            spot = (n + 0.5) / len(entries) * len(times) - 0.5
            low = min(max(int(spot), 0), len(times) - 1)
            high = min(low + 1, len(times) - 1)
            timed.append((times[low] + (spot - low) * (times[high] - times[low]), len(timed), entry))

    own = {step: [("own", step, n) for n in range(nj)] for step in range(1, STEPS + 1)}
    diag = {step: [("diag", step, n) for n in range(nj)] for step in range(1, STEPS + 1)}
    passes = [[("pass", step, j) for j in range(half)] for step in range(STEPS)]
    spread(FILL[0], [("in", 1, part) for part in first])
    spread(FILL[1], [("in", 2, part) for part in first])
    spread(FILL[2], [("in", 3, part) for part in first])
    for step in range(STEPS):
        spread(PASS[step], passes[step])
        spread(EDGE[step][OWN], own[step + 1])
        spread(EDGE[step][DIAG], diag[step + 1])
    spread([7.25], [("late",)])
    spread([STRIPS[0]], [("strips", 2)])
    spread([STRIPS[1]], [("strips", 3)])
    for n, part in enumerate(last):
        rim = part in (0, parts - 1)
        spread([STATS[rim] + 0.01 * n], [("stats", part)])
        spread([ADVANCE[rim] + 0.01 * n], [("advance", part)])
    return [entry for _, _, entry in sorted(timed, key=lambda spot: spot[:2])]


def finish_kernel(field, scaled, mean_ref, scale_ref, scaled_hbm, field_hbm, rims, field_sem, scaled_sem):
    nj, ni, nk, lanes = scaled_hbm.shape
    inner = pl.ds(1, ni - 2)
    for j in range(nj):
        pltpu.make_async_copy(field.at[j + 1, pl.ds(1, ni)], field_hbm.at[j], field_sem).start()
        pltpu.make_async_copy(scaled.at[j, inner], scaled_hbm.at[j, inner], scaled_sem).start()
    places = edge_places(lax.axis_index("cols"), ni)
    for which in (OWN, DIAG):
        for j in range(nj):
            row = pl.ds(which * nj + j, 1)
            mean = jnp.broadcast_to(mean_ref[row, :], (8, lanes))
            scale = jnp.broadcast_to(scale_ref[row, :], (8, lanes))
            for g in range(nk // 8):
                k = pl.ds(8 * g, 8)
                rims[which, j, k, :] = (field[j + 1, places[which], k, :] - mean) * scale
        pltpu.make_async_copy(rims.at[which], scaled_hbm.at[:, places[which] - 1], scaled_sem).start()
    pltpu.make_async_copy(scaled, scaled_hbm, scaled_sem).wait()
    pltpu.make_async_copy(field.at[pl.ds(1, nj), pl.ds(1, ni)], field_hbm, field_sem).wait()


def shards(counts, relay, field_now, earlier, speed_square):
    nj, ni, nk, lanes = field_now.shape
    n_slabs = counts["slabs"]
    levels = n_slabs.bit_length() - 1
    assert n_slabs == 2**levels and levels >= 1
    relay = relay and nj > 1
    parts = line_parts(ni)
    f32 = jnp.float32
    padded = (nj + 2, ni + 2, nk, lanes)
    hbm = pl.BlockSpec(memory_space=pltpu.HBM)
    vmem = pl.BlockSpec(memory_space=pltpu.VMEM)
    cells = nj * ni * nk * lanes
    dma = pltpu.SemaphoreType.DMA
    field, scaled, mean, scale = pl.pallas_call(
        functools.partial(march_kernel, counts, relay),
        name="march",
        out_shape=(
            pltpu.VMEM(padded, f32),
            pltpu.VMEM((nj, ni, nk, lanes), f32),
            pltpu.VMEM((2 * nj, lanes), f32),
            pltpu.VMEM((2 * nj, lanes), f32),
        ),
        in_specs=[hbm] * 3,
        out_specs=(vmem,) * 4,
        scratch_shapes=[
            pltpu.VMEM(padded, f32),
            pltpu.VMEM((STEPS, 2, ni, nj, lanes), f32),
            pltpu.VMEM((STEPS, 2, ni, nj, lanes), f32),
            pltpu.VMEM((STEPS, 2, 2, nj, 1, lanes), f32),
            pltpu.VMEM((STEPS, 2, 2, nj, 1, lanes), f32),
            pltpu.VMEM((levels, 2, nj, ni, lanes), f32),
            pltpu.VMEM((2, 2 * nj, lanes), f32),
            pltpu.VMEM((levels, 2, nj, ni, lanes), f32),
            pltpu.VMEM((n_slabs - 1, 2, 2 * nj, lanes), f32),
            pltpu.VMEM((STEPS, max(nj // 2, 1), nk, lanes), f32),
            pltpu.VMEM((nj, ni, lanes), f32),
            pltpu.VMEM((nj, ni, lanes), f32),
            dma((parts,)),
            dma((parts,)),
            dma((parts,)),
            dma((2, 2)),
            dma((2, 2, nj)),
            dma(()),
            dma((2, max(nj // 2, 1))),
            dma((2, 2)),
            dma((2 * parts + 2,)),
            dma((2, 2)),
            dma((2, 2, 2)),
            dma((2,)),
            dma((2 * parts + 2,)),
            dma((2,)),
            dma((2, 2, nj)),
            dma(()),
            dma((parts, levels)),
            dma(()),
            dma(()),
        ],
        compiler_params=pltpu.CompilerParams(
            collective_id=0, has_side_effects=True, vmem_limit_bytes=40 * 2**20
        ),
        cost_estimate=pl.CostEstimate(flops=33 * cells, bytes_accessed=12 * cells, transcendentals=0),
    )(field_now, earlier, speed_square)
    return pl.pallas_call(
        finish_kernel,
        name="finish",
        out_shape=(jax.ShapeDtypeStruct(field_now.shape, f32),) * 2,
        in_specs=[vmem] * 4,
        out_specs=(hbm,) * 2,
        scratch_shapes=[
            pltpu.VMEM((2, nj, nk, lanes), f32),
            dma(()),
            dma(()),
        ],
        compiler_params=pltpu.CompilerParams(vmem_limit_bytes=16 * 2**20),
        cost_estimate=pl.CostEstimate(flops=2 * cells, bytes_accessed=8 * cells, transcendentals=0),
    )(field, scaled, mean, scale)


def crosses(mesh):
    order = ("rows", "cols", "slabs")
    devices = mesh.devices.transpose([mesh.axis_names.index(axis) for axis in order])
    if devices.shape[1] != 4:
        return False
    one, other = (getattr(devices[0, place, 0], "coords", None) for place in (1, 2))
    return one is not None and sum(a != b for a, b in zip(one, other)) > 1


def solution(mesh):
    spec = P("rows", "cols", "slabs", None)
    return jax.shard_map(
        functools.partial(shards, dict(mesh.shape), crosses(mesh)),
        mesh=mesh,
        in_specs=(spec,) * 3,
        out_specs=(spec,) * 2,
        check_vma=False,
    )
```

```python
import functools

import jax
import jax.numpy as jnp
from jax import lax
from jax.experimental import pallas as pl
from jax.experimental.pallas import tpu as pltpu
from jax.sharding import PartitionSpec as P

STEPS = 3
EPS = 1e-4
MESH = pl.DeviceIdType.MESH
AXES = ("rows", "cols", "slabs")
OWN, DIAG = 0, 1
FILL = ((6.7, 8.0, 8.8, 9.7), (10.5, 11.3, 12.5, 13.3), (14.2, 15.0, 16.3, 17.7))
PASS = ((6.0, 7.4), (14.05, 17.1), (23.2, 26.0))
EDGE = (
    ((7.65, 7.7, 8.75, 13.25), (10.2, 13.2, 12.45, 13.95)),
    ((17.15, 17.2, 17.65, 22.95), (19.1, 22.1, 19.9, 22.9)),
    ((23.6, 25.1, 26.6, 31.1), (28.1, 31.0, 28.9, 30.4)),
)
STRIPS = (14.0, 23.0)
STATS = (19.0, 23.05)
ADVANCE = (23.15, 26.7)


def line_parts(ni):
    return 4 if ni % 32 == 0 else 1


def edge_places(cols, ni):
    odd = lax.rem(cols, 2)
    return ni - odd * (ni - 1), 1 + odd * (ni - 1)


def march_kernel(
    counts, relay, now_hbm, old_hbm, speed_hbm, field, scaled, mean_ref, scale_ref,
    work, face_out, face_in, rim_out, rim_in, own_stats, own_edge, in_stats, all_edge, relayed,
    means, scales, load_rim, load_x, load_y, load_c,
    side_send, side_recv, pass_send, pass_recv, row_send, row_recv, row_rim_recv,
    slab_send, slab_recv, slab_rim_recv, stat_send, edge_send, edge_recv,
):
    nj, ni, nk, lanes = now_hbm.shape
    speed = scaled
    n_slabs = counts["slabs"]
    parts = line_parts(ni)
    width = ni // parts
    inside_out = [0, *range(parts - 1, 0, -1)]
    outside_in = inside_out[2:] + inside_out[:2]
    here = {axis: lax.axis_index(axis) for axis in AXES}
    has_low = {axis: here[axis] > 0 for axis in AXES}
    has_high = {axis: here[axis] < counts[axis] - 1 for axis in AXES}
    odd = lax.rem(here["cols"], 2)
    places = edge_places(here["cols"], ni)
    beside = (here["cols"] + 1 - 2 * odd, here["cols"] - 1 + 2 * odd)
    has_side = tuple((other >= 0) & (other < counts["cols"]) for other in beside)
    halos = ((1 - odd) * (ni + 1), odd * (ni + 1))

    def span(part):
        return part * width, (part + 1) * width

    def load(name, part):
        start, stop = span(part)
        if name == "now":
            start, stop = max(start, 1), min(stop, ni - 1)
        plain, padded = pl.ds(start, stop - start), (pl.ds(1, nj), pl.ds(1 + start, stop - start))
        source, target, sem = {
            "now": (now_hbm, work.at[padded], load_x),
            "old": (old_hbm, field.at[padded], load_y),
            "speed": (speed_hbm, speed.at[:, plain], load_c),
        }[name]
        return pltpu.make_async_copy(source.at[:, plain], target, sem.at[part])

    for place in (0, ni - 1):
        pltpu.make_async_copy(now_hbm.at[:, place], work.at[pl.ds(1, nj), place + 1], load_rim).start()
    for part in inside_out:
        load("now", part).start()
    for part in inside_out[:2]:
        load("old", part).start()
        load("speed", part).start()

    barrier = pltpu.get_barrier_semaphore()
    expected = jnp.int32(0)
    greeted = [("cols", has_side[which], beside[which]) for which in ((OWN,) if relay else (OWN, DIAG))]
    for axis in ("rows", "slabs"):
        greeted += [(axis, has_low[axis], here[axis] - 1), (axis, has_high[axis], here[axis] + 1)]
    for axis, there, target in greeted:
        expected = expected + there.astype(jnp.int32)

        @pl.when(there)
        def _():
            pl.semaphore_signal(barrier, inc=1, device_id={axis: target}, device_id_type=MESH)

    peers = [lax.rem(here["slabs"] + gap, n_slabs) for gap in range(1, n_slabs)]
    if relay:
        over = lax.rem(here["cols"] + 2, 4)
        pl.semaphore_signal(barrier, inc=1, device_id={"cols": over}, device_id_type=MESH)
        expected = expected + 1
    pl.semaphore_wait(barrier, expected)
    for part in inside_out[2:]:
        load("old", part).start()
        load("speed", part).start()

    half = nj // 2 if relay else 0
    relays = has_side[OWN] & ~has_side[DIAG]

    def buffer_of(step):
        return work if step % 2 == 0 else field

    def remote(source, landing, send, recv, axis, target):
        return pltpu.make_async_remote_copy(
            source, landing, send, recv, device_id={axis: target}, device_id_type=MESH
        )

    def directions(axis):
        for to_high in (0, 1):
            yield to_high, has_high[axis] if to_high else has_low[axis], here[axis] + (1 if to_high else -1)

    def taken(axis, one, two):
        pl.when(has_low[axis] & has_high[axis])(two.wait_recv)
        pl.when(has_low[axis] ^ has_high[axis])(one.wait_recv)

    def side_copy(step, which, j, kind="straight"):
        buffer = buffer_of(step)
        source, target = buffer.at[j + 1, places[which]], beside[which]
        landing = buffer.at[j + 1, ni + 1 - halos[which]]
        sems = side_send.at[step % 2, which], side_recv.at[step % 2, which, j]
        if kind == "to":
            landing, target = relayed.at[step, j], over
            sems = sems[0], pass_recv.at[step % 2, j]
        elif kind == "on":
            source, landing, target = relayed.at[step, j], buffer.at[j + 1, halos[OWN]], beside[OWN]
            sems = pass_send, sems[1]
        return remote(source, landing, *sems, "cols", target)

    def side(step, which, j, what):
        relayed_line = which == DIAG and j < half
        if what == "start":
            held = half and which == OWN and j == nj - 1
            there = has_side[which] & ~relays if held else has_side[which]
            pl.when(there)(side_copy(step, which, j, "to" if relayed_line else "straight").start)
        else:
            pl.when(has_side[which])(side_copy(step, which, j).wait_recv)

    def side_sent(step, which):
        lines = buffer_of(step).at[pl.ds(1, nj), places[which]]
        copy = remote(lines, lines, side_send.at[step % 2, which], side_recv.at[step % 2, which, 0], "cols", beside[which])
        pl.when(has_side[which])(copy.wait_send)

    def hand_on(step, j):
        @pl.when(relays)
        def _():
            side_copy(step, DIAG, j, "to").wait_recv()
            side_copy(step, DIAG, j, "on").start()
            if j == 0:
                side_copy(step, OWN, nj - 1).start()

    def segment(step, number):
        if number < parts:
            start, stop = span(number)
            rim = 1 if step < 2 else 2
            return max(1 + start, 1 + rim), min(1 + stop, 1 + ni - rim)
        place = 2 if number == parts else ni - 1
        return place, place + 1

    def slot(step, number):
        return step % 2 * parts + number if number < parts else parts + number

    def rows(step, number, what):
        start, stop = segment(step, number)
        lines, buffer, recv = pl.ds(start, stop - start), buffer_of(step), row_recv.at[slot(step, number)]
        if what == "taken":
            one, two = (buffer.at[pl.ds(0, n), lines] for n in (1, 2))
            send = row_send.at[step % 2, 0]
            taken("rows", *(remote(some, some, send, recv, "rows", here["rows"]) for some in (one, two)))
            return
        for to_high, there, target in directions("rows"):
            source, landing = (nj, 0) if to_high else (1, nj + 1)
            copy = remote(
                buffer.at[source, lines], buffer.at[landing, lines], row_send.at[step % 2, to_high], recv, "rows", target
            )
            pl.when(there)(copy.start)

    def rows_sent(step):
        for to_high, there, target in directions("rows"):
            lines = buffer_of(step).at[nj if to_high else 1, pl.ds(1, ni)]
            copy = remote(lines, lines, row_send.at[step % 2, to_high], row_recv.at[0], "rows", target)
            pl.when(there)(copy.wait_send)

    def row_rim(step, which, to_highs, what):
        buffer = buffer_of(step)
        for to_high, there, target in directions("rows"):
            if to_high not in to_highs:
                continue
            source, landing = (nj, 0) if to_high else (1, nj + 1)
            copy = remote(
                buffer.at[source, places[which]], buffer.at[landing, places[which]],
                row_send.at[step % 2, to_high], row_rim_recv.at[step % 2, to_high, which], "rows", target,
            )
            if what == "start":
                pl.when(there)(copy.start)
            else:
                pl.when(has_low["rows"] if to_high else has_high["rows"])(copy.wait_recv)

    def slabs(step, number, what):
        start, stop = segment(step, number)
        lines, recv = pl.ds(start - 1, stop - start), slab_recv.at[slot(step, number)]
        if what == "taken":
            one, two = (face_in.at[step, pl.ds(0, n), lines] for n in (1, 2))
            taken("slabs", *(remote(some, some, slab_send.at[0], recv, "slabs", here["slabs"]) for some in (one, two)))
            return
        for to_high, there, target in directions("slabs"):
            copy = remote(
                face_out.at[step, to_high, lines], face_in.at[step, to_high, lines],
                slab_send.at[to_high], recv, "slabs", target,
            )
            pl.when(there)(copy.start)

    def slab_rim(step, which, j, what):
        recv = slab_rim_recv.at[step % 2, which, j]
        if what == "taken":
            one, two = (rim_in.at[step, pl.ds(0, n), which, j] for n in (1, 2))
            taken("slabs", *(remote(some, some, slab_send.at[0], recv, "slabs", here["slabs"]) for some in (one, two)))
            return
        for to_high, there, target in directions("slabs"):
            copy = remote(
                rim_out.at[step, to_high, which, j], rim_in.at[step, to_high, which, j],
                slab_send.at[to_high], recv, "slabs", target,
            )
            pl.when(there)(copy.start)

    def slabs_sent():
        for to_high, there, target in directions("slabs"):
            sent = face_out.at[:, to_high]
            pl.when(there)(remote(sent, sent, slab_send.at[to_high], slab_recv.at[0], "slabs", target).wait_send)

    pltpu.make_async_copy(now_hbm.at[:, pl.ds(0, 2)], work.at[pl.ds(1, nj), pl.ds(1, 2)], load_rim).wait()
    for j in range(half):
        side(0, DIAG, j, "start")
    for j in range(nj):
        side(0, OWN, j, "start")
    if not half:
        for j in range(nj):
            side(0, DIAG, j, "start")
    for which in (OWN, DIAG):
        for j in range(nj):
            rim_out[0, 0, which, j] = work[j + 1, places[which], pl.ds(0, 1), :]
            rim_out[0, 1, which, j] = work[j + 1, places[which], pl.ds(nk - 1, 1), :]
    for which in (OWN, DIAG):
        row_rim(0, which, (0, 1), "start")
        for j in range(nj):
            slab_rim(0, which, j, "start")

    zeros_line = jnp.zeros((nk, lanes), jnp.float32)
    for buffer in (work, field):
        for absent, edge in ((~has_low["rows"], 0), (~has_high["rows"], nj + 1)):
            @pl.when(absent)
            def _():
                @pl.loop(1, ni + 1)
                def _(i):
                    buffer[edge, i] = zeros_line
        for absent, edge in ((~has_low["cols"], 0), (~has_high["cols"], ni + 1)):
            @pl.when(absent)
            def _():
                @pl.loop(1, nj + 1)
                def _(j):
                    buffer[j, edge] = zeros_line
    for absent, to_high in ((~has_low["slabs"], 1), (~has_high["slabs"], 0)):
        @pl.when(absent)
        def _():
            for step in range(STEPS):
                face_in[step, to_high] = jnp.zeros((ni, nj, lanes), jnp.float32)
                rim_in[step, to_high] = jnp.zeros((2, nj, 1, lanes), jnp.float32)
    own_stats[...] = jnp.zeros_like(own_stats)

    for part in inside_out:
        load("now", part).wait()
        rows(0, part, "start")
        start, stop = segment(0, part)

        @pl.loop(start, stop)
        def _(i):
            for j in range(nj):
                face_out[0, 0, i - 1, pl.ds(j, 1), :] = work[j + 1, i, pl.ds(0, 1), :]
                face_out[0, 1, i - 1, pl.ds(j, 1), :] = work[j + 1, i, pl.ds(nk - 1, 1), :]

        slabs(0, part, "start")

    groups = nk // 8
    row_number = lax.broadcasted_iota(jnp.int32, (8, lanes), 0)

    def line(step, i, js, rim=None):
        now, old = (work, field) if step % 2 == 1 else (field, work)
        last = step == STEPS
        sums = {}

        def halo(to_high, j):
            if rim is None:
                return face_in[step - 1, to_high, i - 1, pl.ds(j, 1), :]
            return rim_in[step - 1, to_high, rim, j]

        def keep(to_high, j, row):
            if rim is None:
                face_out[step, to_high, i - 1, pl.ds(j, 1), :] = row
            else:
                rim_out[step, to_high, rim, j] = row

        for g in range(groups):
            k = pl.ds(8 * g, 8)
            column = {j: now[j, i, k, :] for j in range(js[0], js[-1] + 3)}
            for j in js:
                middle = column[j + 1]
                if g == 0:
                    low = jnp.where(
                        row_number == 0, jnp.broadcast_to(halo(1, j), (8, lanes)), pltpu.roll(middle, 1, 0)
                    )
                else:
                    low = now[j + 1, i, pl.ds(8 * g - 1, 8), :]
                if g == groups - 1:
                    high = jnp.where(
                        row_number == 7, jnp.broadcast_to(halo(0, j), (8, lanes)), pltpu.roll(middle, 7, 0)
                    )
                else:
                    high = now[j + 1, i, pl.ds(8 * g + 1, 8), :]
                spread = (
                    (column[j] + column[j + 2])
                    + (now[j + 1, i - 1, k, :] + now[j + 1, i + 1, k, :])
                    + (low + high)
                    - 6.0 * middle
                )
                later = 2.0 * middle - old[j + 1, i, k, :] + speed[j, i - 1, k, :] * spread
                old[j + 1, i, k, :] = later
                if last:
                    sums[j] = later if g == 0 else sums[j] + later
                else:
                    if g == 0:
                        keep(0, j, later[0:1])
                    if g == groups - 1:
                        keep(1, j, later[7:8])
        if last:
            for j in js:
                total = jnp.sum(sums[j], axis=0, keepdims=True)
                mean = jnp.broadcast_to(total * (1.0 / nk), (8, lanes))
                squares = None
                for g in range(groups):
                    moved = old[j + 1, i, pl.ds(8 * g, 8), :] - mean
                    squares = moved * moved if g == 0 else squares + moved * moved
                square = jnp.sum(squares, axis=0, keepdims=True)
                if rim is None:
                    own_stats[0, 0, j, pl.ds(i - 1, 1), :] = total
                    own_stats[0, 1, j, pl.ds(i - 1, 1), :] = square
                else:
                    own_edge[0, pl.ds(rim * nj + j, 1), :] = total
                    own_edge[1, pl.ds(rim * nj + j, 1), :] = square

    every_j, begun = tuple(range(nj)), set()

    def loaded(part):
        if ("load", part) not in begun:
            begun.add(("load", part))
            load("old", part).wait()
            load("speed", part).wait()

    def interior(step, part):
        start, stop = span(part)
        rim = max(step, 1)
        start, stop = max(1 + start, 1 + rim), min(1 + stop, 1 + ni - rim)
        if step == 1:
            loaded(part)
        rows(step - 1, part, "taken")
        slabs(step - 1, part, "taken")
        if step >= 2 and step not in begun:
            begun.add(step)
            rows_sent(step - 2)

        @pl.loop(start, stop)
        def _(i):
            line(step, i, every_j)

        if step < STEPS:
            rows(step, part, "start")
            slabs(step, part, "start")

    def strips(step):
        if step == 2:
            for number, place in ((parts, 2), (parts + 1, ni - 1)):
                line(step, place, every_j)
                rows(step, number, "start")
                slabs(step, number, "start")
        else:
            for number in (parts, parts + 1):
                rows(step - 1, number, "taken")
                slabs(step - 1, number, "taken")
            for place in (3, ni - 2, 2, ni - 1):
                line(step, place, every_j)

    def edge(step, which, j):
        side(step - 1, which, j, "taken")
        slab_rim(step - 1, which, j, "taken")
        shared = [to_high for to_high, place in ((0, 0), (1, nj - 1)) if place == j]
        row_rim(step - 1, which, [1 - to_high for to_high in shared], "taken")
        if step >= 2 and (step, which) not in begun:
            begun.add((step, which))
            side_sent(step - 2, which)
        if step == 1:
            loaded(0)
            loaded(parts - 1)
        line(step, places[which], (j,), which)
        if half and (step, which, j) == (1, OWN, 0):
            for other in range(half, nj):
                side(0, DIAG, other, "start")
        if step < STEPS:
            side(step, which, j, "start")
            slab_rim(step, which, j, "start")
            row_rim(step, which, shared, "start")

    levels = n_slabs.bit_length() - 1
    stat_recv = (load_x, load_y, load_c)
    partners = []
    for level in range(levels):
        bit = lax.rem(here["slabs"] // 2**level, 2)
        partners.append(here["slabs"] + (1 - 2 * bit) * 2**level)

    def stat_copy(part, level):
        lines = pl.ds(part * width, width)
        return remote(
            own_stats.at[level, :, :, lines], in_stats.at[level, :, :, lines],
            stat_send, stat_recv[level].at[part], "slabs", partners[level],
        )

    def merged(part, level):
        lines = pl.ds(part * width, width)
        stat_copy(part, level).wait_recv()
        mine, theirs = own_stats[level, :, :, lines, :], in_stats[level, :, :, lines, :]
        cells = float(nk * 2**level)
        apart = (theirs[0] - mine[0]) * (1.0 / cells)
        return mine[0] + theirs[0], mine[1] + theirs[1] + (0.5 * cells) * apart * apart

    def advance(part, level):
        lines = pl.ds(part * width, width)
        total, square = merged(part, level)
        own_stats[level + 1, 0, :, lines, :] = total
        own_stats[level + 1, 1, :, lines, :] = square
        stat_copy(part, level + 1).start()

    whole = float(nk * n_slabs)

    def rescale(part):
        lines = pl.ds(part * width, width)
        total, square = merged(part, levels - 1)
        means[:, lines, :] = total * (1.0 / whole)
        scales[:, lines, :] = lax.rsqrt(square * (1.0 / whole) + EPS)
        start, stop = span(part)

        @pl.loop(max(start, 1), min(stop, ni - 1))
        def _(i):
            for j in range(nj):
                mean = jnp.broadcast_to(means[j, pl.ds(i, 1), :], (8, lanes))
                scale = jnp.broadcast_to(scales[j, pl.ds(i, 1), :], (8, lanes))
                for g in range(groups):
                    k = pl.ds(8 * g, 8)
                    scaled[j, i, k, :] = (field[j + 1, i + 1, k, :] - mean) * scale

    def do(kind, *what):
        if kind == "in":
            interior(what[0], what[1])
        elif kind == "own":
            edge(what[0], OWN, what[1])
        elif kind == "diag":
            edge(what[0], DIAG, what[1])
        elif kind == "pass":
            hand_on(*what)
        elif kind == "strips":
            strips(what[0])
        elif kind == "stats":
            stat_copy(what[0], 0).start()
        elif kind == "advance":
            for level in range(levels - 1):
                advance(what[0], level)
        elif kind == "rescale":
            rescale(what[0])

    for what in agenda(nj, half, parts, inside_out, outside_in):
        do(*what)

    gaps = range(1, n_slabs)
    for gap in gaps:
        remote(own_edge, all_edge.at[gap - 1], edge_send, edge_recv, "slabs", peers[gap - 1]).start()
    for part in outside_in:
        rescale(part)

    def combine(own, others):
        mean = own[0]
        for other in others:
            mean = mean + other[0]
        mean = mean * (1.0 / whole)
        square = None
        for one in (own, *others):
            gap = one[0] * (1.0 / nk) - mean
            term = one[1] + nk * gap * gap
            square = term if square is None else square + term
        return mean, lax.rsqrt(square * (1.0 / whole) + EPS)

    for step in range(STEPS):
        if step == 2:
            for which in (OWN, DIAG):
                side_sent(step, which)
            rows_sent(step)
    slabs_sent()
    if half:
        pl.when(relays)(remote(relayed, relayed, pass_send, pass_recv.at[0, 0], "cols", beside[OWN]).wait_send)
    remote(own_stats, in_stats, stat_send, stat_recv[0].at[0], "slabs", partners[0]).wait_send()
    edges = remote(all_edge, all_edge, edge_send, edge_recv, "slabs", peers[0])
    edges.wait_recv()
    mean, scale = combine(own_edge[...], [all_edge[gap - 1] for gap in gaps])
    mean_ref[...] = mean
    scale_ref[...] = scale
    edges.wait_send()


def agenda(nj, half, parts, first, last):
    timed = []

    def spread(times, entries):
        for n, entry in enumerate(entries):
            spot = min(max((n + 0.5) / len(entries) * len(times) - 0.5, 0), len(times) - 1)
            low = int(spot)
            high = min(low + 1, len(times) - 1)
            timed.append((times[low] + (spot - low) * (times[high] - times[low]), len(timed), entry))

    own = {step: [("own", step, n) for n in range(nj)] for step in range(1, STEPS + 1)}
    diag = {step: [("diag", step, n) for n in range(nj)] for step in range(1, STEPS + 1)}
    passes = [[("pass", step, j) for j in range(half)] for step in range(STEPS)]
    spread(FILL[0], [("in", 1, part) for part in first])
    spread(FILL[1], [("in", 2, part) for part in first])
    spread(FILL[2], [("in", 3, part) for part in first])
    for step in range(STEPS):
        spread(PASS[step], passes[step])
        spread(EDGE[step][OWN], own[step + 1])
        spread(EDGE[step][DIAG], diag[step + 1])
    spread([STRIPS[0]], [("strips", 2)])
    spread([STRIPS[1]], [("strips", 3)])
    for n, part in enumerate(last):
        rim = part in (0, parts - 1)
        spread([STATS[rim] + 0.01 * n], [("stats", part)])
        spread([ADVANCE[rim] + 0.01 * n], [("advance", part)])
    return [entry for _, _, entry in sorted(timed, key=lambda spot: spot[:2])]


def finish_kernel(field, scaled, mean_ref, scale_ref, scaled_hbm, field_hbm, rims, field_sem, scaled_sem):
    nj, ni, nk, lanes = scaled_hbm.shape
    inner = pl.ds(1, ni - 2)
    for j in range(nj):
        pltpu.make_async_copy(field.at[j + 1, pl.ds(1, ni)], field_hbm.at[j], field_sem).start()
        pltpu.make_async_copy(scaled.at[j, inner], scaled_hbm.at[j, inner], scaled_sem).start()
    places = edge_places(lax.axis_index("cols"), ni)
    for which in (OWN, DIAG):
        for j in range(nj):
            row = pl.ds(which * nj + j, 1)
            mean = jnp.broadcast_to(mean_ref[row, :], (8, lanes))
            scale = jnp.broadcast_to(scale_ref[row, :], (8, lanes))
            for g in range(nk // 8):
                k = pl.ds(8 * g, 8)
                rims[which, j, k, :] = (field[j + 1, places[which], k, :] - mean) * scale
        pltpu.make_async_copy(rims.at[which], scaled_hbm.at[:, places[which] - 1], scaled_sem).start()
    pltpu.make_async_copy(scaled, scaled_hbm, scaled_sem).wait()
    pltpu.make_async_copy(field.at[pl.ds(1, nj), pl.ds(1, ni)], field_hbm, field_sem).wait()


def shards(counts, relay, field_now, earlier, speed_square):
    nj, ni, nk, lanes = field_now.shape
    n_slabs = counts["slabs"]
    levels = n_slabs.bit_length() - 1
    assert n_slabs == 2**levels and 1 <= levels <= 3
    relay = relay and nj > 1
    parts = line_parts(ni)
    f32 = jnp.float32
    padded = (nj + 2, ni + 2, nk, lanes)
    hbm = pl.BlockSpec(memory_space=pltpu.HBM)
    vmem = pl.BlockSpec(memory_space=pltpu.VMEM)
    cells = nj * ni * nk * lanes
    dma = pltpu.SemaphoreType.DMA
    field, scaled, mean, scale = pl.pallas_call(
        functools.partial(march_kernel, counts, relay),
        name="march",
        out_shape=(
            pltpu.VMEM(padded, f32),
            pltpu.VMEM((nj, ni, nk, lanes), f32),
            pltpu.VMEM((2 * nj, lanes), f32),
            pltpu.VMEM((2 * nj, lanes), f32),
        ),
        in_specs=[hbm] * 3,
        out_specs=(vmem,) * 4,
        scratch_shapes=[
            pltpu.VMEM(padded, f32),
            pltpu.VMEM((STEPS, 2, ni, nj, lanes), f32),
            pltpu.VMEM((STEPS, 2, ni, nj, lanes), f32),
            pltpu.VMEM((STEPS, 2, 2, nj, 1, lanes), f32),
            pltpu.VMEM((STEPS, 2, 2, nj, 1, lanes), f32),
            pltpu.VMEM((levels, 2, nj, ni, lanes), f32),
            pltpu.VMEM((2, 2 * nj, lanes), f32),
            pltpu.VMEM((levels, 2, nj, ni, lanes), f32),
            pltpu.VMEM((n_slabs - 1, 2, 2 * nj, lanes), f32),
            pltpu.VMEM((STEPS, max(nj // 2, 1), nk, lanes), f32),
            pltpu.VMEM((nj, ni, lanes), f32),
            pltpu.VMEM((nj, ni, lanes), f32),
            dma(()),
            dma((parts,)),
            dma((parts,)),
            dma((parts,)),
            dma((2, 2)),
            dma((2, 2, nj)),
            dma(()),
            dma((2, max(nj // 2, 1))),
            dma((2, 2)),
            dma((2 * parts + 2,)),
            dma((2, 2, 2)),
            dma((2,)),
            dma((2 * parts + 2,)),
            dma((2, 2, nj)),
            dma(()),
            dma(()),
            dma(()),
        ],
        compiler_params=pltpu.CompilerParams(
            collective_id=0, has_side_effects=True, vmem_limit_bytes=40 * 2**20
        ),
        cost_estimate=pl.CostEstimate(flops=33 * cells, bytes_accessed=12 * cells, transcendentals=0),
    )(field_now, earlier, speed_square)
    return pl.pallas_call(
        finish_kernel,
        name="finish",
        out_shape=(jax.ShapeDtypeStruct(field_now.shape, f32),) * 2,
        in_specs=[vmem] * 4,
        out_specs=(hbm,) * 2,
        scratch_shapes=[
            pltpu.VMEM((2, nj, nk, lanes), f32),
            dma(()),
            dma(()),
        ],
        compiler_params=pltpu.CompilerParams(vmem_limit_bytes=16 * 2**20),
        cost_estimate=pl.CostEstimate(flops=2 * cells, bytes_accessed=8 * cells, transcendentals=0),
    )(field, scaled, mean, scale)


def crosses(mesh):
    order = ("rows", "cols", "slabs")
    devices = mesh.devices.transpose([mesh.axis_names.index(axis) for axis in order])
    if devices.shape[1] != 4:
        return False
    one, other = (getattr(devices[0, place, 0], "coords", None) for place in (1, 2))
    return one is not None and sum(a != b for a, b in zip(one, other)) > 1


def solution(mesh):
    spec = P("rows", "cols", "slabs", None)
    return jax.shard_map(
        functools.partial(shards, dict(mesh.shape), crosses(mesh)),
        mesh=mesh,
        in_specs=(spec,) * 3,
        out_specs=(spec,) * 2,
        check_vma=False,
    )
```

```python
import functools

import jax
import jax.numpy as jnp
from jax import lax
from jax.experimental import pallas as pl
from jax.experimental.pallas import tpu as pltpu
from jax.sharding import PartitionSpec as P

STEPS = 3
EPS = 1e-4
MESH = pl.DeviceIdType.MESH
AXES = ("rows", "cols", "slabs")
OWN, DIAG = 0, 1
FILL = ((6.7, 8.0, 8.8, 9.7), (10.5, 11.3, 12.5, 13.3), (14.2, 15.0, 16.3, 17.7))
PASS = ((6.0, 7.4), (14.05, 17.1), (23.2, 26.0))
EDGE = (
    ((7.65, 7.7, 8.75, 13.25), (10.2, 13.2, 12.45, 13.95)),
    ((17.15, 17.2, 17.65, 19.5), (19.1, 22.1, 19.9, 22.9)),
    ((23.6, 25.1, 26.6, 29.5), (28.1, 31.0, 30.3, 31.8)),
)
STRIPS = (14.0, 23.0)
STATS = (19.0, 23.05)
ADVANCE = (23.7, 26.7)


def line_parts(ni):
    return 4 if ni % 32 == 0 else 1


def edge_places(cols, ni):
    odd = lax.rem(cols, 2)
    return ni - odd * (ni - 1), 1 + odd * (ni - 1)


def march_kernel(
    counts, relay, now_hbm, old_hbm, speed_hbm, field, scaled, own_edge, all_edge,
    work, face_out, face_in, rim_out, rim_in, own_stats, in_stats, relayed,
    means, scales, load_rim, load_x, load_y, load_c,
    side_send, side_recv, pass_send, row_send, row_recv, row_rim_recv,
    slab_send, slab_recv, slab_rim_recv, stat_send, edge_send, edge_recv,
):
    nj, ni, nk, lanes = now_hbm.shape
    speed = scaled
    n_slabs = counts["slabs"]
    parts = line_parts(ni)
    width = ni // parts
    inside_out = [0, *range(parts - 1, 0, -1)]
    outside_in = inside_out[2:] + inside_out[:2]
    here = {axis: lax.axis_index(axis) for axis in AXES}
    has_low = {axis: here[axis] > 0 for axis in AXES}
    has_high = {axis: here[axis] < counts[axis] - 1 for axis in AXES}
    odd = lax.rem(here["cols"], 2)
    places = edge_places(here["cols"], ni)
    beside = (here["cols"] + 1 - 2 * odd, here["cols"] - 1 + 2 * odd)
    has_side = tuple((other >= 0) & (other < counts["cols"]) for other in beside)
    halos = ((1 - odd) * (ni + 1), odd * (ni + 1))

    def span(part):
        return part * width, (part + 1) * width

    def load(name, part):
        start, stop = span(part)
        if name == "now":
            start, stop = max(start, 1), min(stop, ni - 1)
        plain, padded = pl.ds(start, stop - start), (pl.ds(1, nj), pl.ds(1 + start, stop - start))
        source, target, sem = {
            "now": (now_hbm, work.at[padded], load_x),
            "old": (old_hbm, field.at[padded], load_y),
            "speed": (speed_hbm, speed.at[:, plain], load_c),
        }[name]
        return pltpu.make_async_copy(source.at[:, plain], target, sem.at[part])

    for place in (0, ni - 1):
        pltpu.make_async_copy(now_hbm.at[:, place], work.at[pl.ds(1, nj), place + 1], load_rim).start()
    for part in inside_out:
        load("now", part).start()
    for part in inside_out[:2]:
        load("old", part).start()
        load("speed", part).start()

    barrier = pltpu.get_barrier_semaphore()
    expected = jnp.int32(0)
    greeted = [("cols", has_side[which], beside[which]) for which in ((OWN,) if relay else (OWN, DIAG))]
    for axis in ("rows", "slabs"):
        greeted += [(axis, has_low[axis], here[axis] - 1), (axis, has_high[axis], here[axis] + 1)]
    for axis, there, target in greeted:
        expected = expected + there.astype(jnp.int32)

        @pl.when(there)
        def _():
            pl.semaphore_signal(barrier, inc=1, device_id={axis: target}, device_id_type=MESH)

    peers = [lax.rem(here["slabs"] + gap, n_slabs) for gap in range(1, n_slabs)]
    if relay:
        over = lax.rem(here["cols"] + 2, 4)
        pl.semaphore_signal(barrier, inc=1, device_id={"cols": over}, device_id_type=MESH)
        expected = expected + 1
    pl.semaphore_wait(barrier, expected)
    for part in inside_out[2:]:
        load("old", part).start()
        load("speed", part).start()

    half = nj // 2 if relay else 0
    relays = has_side[OWN] & ~has_side[DIAG]

    def buffer_of(step):
        return work if step % 2 == 0 else field

    def remote(source, landing, send, recv, axis, target):
        return pltpu.make_async_remote_copy(
            source, landing, send, recv, device_id={axis: target}, device_id_type=MESH
        )

    def directions(axis):
        for to_high in (0, 1):
            yield to_high, has_high[axis] if to_high else has_low[axis], here[axis] + (1 if to_high else -1)

    def taken(axis, one, two):
        pl.when(has_low[axis] & has_high[axis])(two.wait_recv)
        pl.when(has_low[axis] ^ has_high[axis])(one.wait_recv)

    def side_copy(step, which, j, kind="straight"):
        buffer = buffer_of(step)
        source, target = buffer.at[j + 1, places[which]], beside[which]
        landing = buffer.at[j + 1, ni + 1 - halos[which]]
        sems = side_send.at[step % 2, which], side_recv.at[step % 2, which, j]
        if kind == "to":
            landing, target = relayed.at[step, j], over
            sems = sems[0], side_recv.at[step % 2, DIAG, j]
        elif kind == "on":
            source, landing, target = relayed.at[step, j], buffer.at[j + 1, halos[OWN]], beside[OWN]
            sems = pass_send, sems[1]
        return remote(source, landing, *sems, "cols", target)

    def side(step, which, j, what):
        relayed_line = which == DIAG and j < half
        if what == "start":
            held = half and which == OWN and j == nj - 1
            there = has_side[which] & ~relays if held else has_side[which]
            pl.when(there)(side_copy(step, which, j, "to" if relayed_line else "straight").start)
        else:
            pl.when(has_side[which])(side_copy(step, which, j).wait_recv)

    def side_sent(step, which):
        lines = buffer_of(step).at[pl.ds(1, nj), places[which]]
        copy = remote(lines, lines, side_send.at[step % 2, which], side_recv.at[step % 2, which, 0], "cols", beside[which])
        pl.when(has_side[which])(copy.wait_send)

    def hand_on(step, j):
        @pl.when(relays)
        def _():
            side_copy(step, DIAG, j, "to").wait_recv()
            side_copy(step, DIAG, j, "on").start()
            if j == 0:
                side_copy(step, OWN, nj - 1).start()

    def segment(step, number):
        if number < parts:
            start, stop = span(number)
            rim = 1 if step < 2 else 2
            return max(1 + start, 1 + rim), min(1 + stop, 1 + ni - rim)
        place = 2 if number == parts else ni - 1
        return place, place + 1

    def arrival(sems, strip_sem, step, number):
        return sems.at[step % 2 * parts + number] if number < parts else load_c.at[strip_sem + number - parts]

    def rows(step, number, what):
        start, stop = segment(step, number)
        lines, buffer, recv = pl.ds(start, stop - start), buffer_of(step), arrival(row_recv, 0, step, number)
        if what == "taken":
            one, two = (buffer.at[pl.ds(0, n), lines] for n in (1, 2))
            send = row_send.at[step % 2, 0]
            taken("rows", *(remote(some, some, send, recv, "rows", here["rows"]) for some in (one, two)))
            return
        for to_high, there, target in directions("rows"):
            source, landing = (nj, 0) if to_high else (1, nj + 1)
            copy = remote(
                buffer.at[source, lines], buffer.at[landing, lines], row_send.at[step % 2, to_high], recv, "rows", target
            )
            pl.when(there)(copy.start)

    def rows_sent(step):
        for to_high, there, target in directions("rows"):
            lines = buffer_of(step).at[nj if to_high else 1, pl.ds(1, ni)]
            copy = remote(lines, lines, row_send.at[step % 2, to_high], row_recv.at[0], "rows", target)
            pl.when(there)(copy.wait_send)

    def row_rim(step, which, to_highs, what):
        buffer = buffer_of(step)
        for to_high, there, target in directions("rows"):
            if to_high not in to_highs:
                continue
            source, landing = (nj, 0) if to_high else (1, nj + 1)
            copy = remote(
                buffer.at[source, places[which]], buffer.at[landing, places[which]],
                row_send.at[step % 2, to_high], row_rim_recv.at[step % 2, to_high, which], "rows", target,
            )
            if what == "start":
                pl.when(there)(copy.start)
            else:
                pl.when(has_low["rows"] if to_high else has_high["rows"])(copy.wait_recv)

    def slabs(step, number, what):
        start, stop = segment(step, number)
        lines, recv = pl.ds(start - 1, stop - start), arrival(slab_recv, 2, step, number)
        if what == "taken":
            one, two = (face_in.at[step, pl.ds(0, n), lines] for n in (1, 2))
            taken("slabs", *(remote(some, some, slab_send.at[0], recv, "slabs", here["slabs"]) for some in (one, two)))
            return
        for to_high, there, target in directions("slabs"):
            copy = remote(
                face_out.at[step, to_high, lines], face_in.at[step, to_high, lines],
                slab_send.at[to_high], recv, "slabs", target,
            )
            pl.when(there)(copy.start)

    group = 2 if nj % 2 == 0 else 1

    def slab_rim(step, which, pair, what):
        recv, j = slab_rim_recv.at[step % 2, which, pair], pl.ds(group * pair, group)
        if what == "taken":
            one, two = (rim_in.at[step, pl.ds(0, n), which, j] for n in (1, 2))
            taken("slabs", *(remote(some, some, slab_send.at[0], recv, "slabs", here["slabs"]) for some in (one, two)))
            return
        for to_high, there, target in directions("slabs"):
            copy = remote(
                rim_out.at[step, to_high, which, j], rim_in.at[step, to_high, which, j],
                slab_send.at[to_high], recv, "slabs", target,
            )
            pl.when(there)(copy.start)

    def slabs_sent():
        for to_high, there, target in directions("slabs"):
            sent = face_out.at[:, to_high]
            pl.when(there)(remote(sent, sent, slab_send.at[to_high], slab_recv.at[0], "slabs", target).wait_send)

    pltpu.make_async_copy(now_hbm.at[:, pl.ds(0, 2)], work.at[pl.ds(1, nj), pl.ds(1, 2)], load_rim).wait()
    for j in range(half):
        side(0, DIAG, j, "start")
    for j in range(nj):
        side(0, OWN, j, "start")
    if not half:
        for j in range(nj):
            side(0, DIAG, j, "start")
    for which in (OWN, DIAG):
        for j in range(nj):
            rim_out[0, 0, which, j] = work[j + 1, places[which], pl.ds(0, 1), :]
            rim_out[0, 1, which, j] = work[j + 1, places[which], pl.ds(nk - 1, 1), :]
    for which in (OWN, DIAG):
        row_rim(0, which, (0, 1), "start")
        for pair in range(nj // group):
            slab_rim(0, which, pair, "start")

    zeros_line = jnp.zeros((nk, lanes), jnp.float32)
    for buffer in (work, field):
        for absent, edge in ((~has_low["rows"], 0), (~has_high["rows"], nj + 1)):
            @pl.when(absent)
            def _():
                @pl.loop(1, ni + 1)
                def _(i):
                    buffer[edge, i] = zeros_line
        for absent, edge in ((~has_low["cols"], 0), (~has_high["cols"], ni + 1)):
            @pl.when(absent)
            def _():
                @pl.loop(1, nj + 1)
                def _(j):
                    buffer[j, edge] = zeros_line
    for absent, to_high in ((~has_low["slabs"], 1), (~has_high["slabs"], 0)):
        @pl.when(absent)
        def _():
            for step in range(STEPS):
                face_in[step, to_high] = jnp.zeros((ni, nj, lanes), jnp.float32)
                rim_in[step, to_high] = jnp.zeros((2, nj, 1, lanes), jnp.float32)
    own_stats[...] = jnp.zeros_like(own_stats)

    for part in inside_out:
        load("now", part).wait()
        rows(0, part, "start")
        start, stop = segment(0, part)

        @pl.loop(start, stop)
        def _(i):
            for j in range(nj):
                face_out[0, 0, i - 1, pl.ds(j, 1), :] = work[j + 1, i, pl.ds(0, 1), :]
                face_out[0, 1, i - 1, pl.ds(j, 1), :] = work[j + 1, i, pl.ds(nk - 1, 1), :]

        slabs(0, part, "start")

    groups = nk // 8
    row_number = lax.broadcasted_iota(jnp.int32, (8, lanes), 0)

    def line(step, i, js, rim=None):
        now, old = (work, field) if step % 2 == 1 else (field, work)
        last = step == STEPS
        sums = {}

        def halo(to_high, j):
            if rim is None:
                return face_in[step - 1, to_high, i - 1, pl.ds(j, 1), :]
            return rim_in[step - 1, to_high, rim, j]

        def keep(to_high, j, row):
            if rim is None:
                face_out[step, to_high, i - 1, pl.ds(j, 1), :] = row
            else:
                rim_out[step, to_high, rim, j] = row

        for g in range(groups):
            k = pl.ds(8 * g, 8)
            column = {j: now[j, i, k, :] for j in range(js[0], js[-1] + 3)}
            for j in js:
                middle = column[j + 1]
                if g == 0:
                    low = jnp.where(
                        row_number == 0, jnp.broadcast_to(halo(1, j), (8, lanes)), pltpu.roll(middle, 1, 0)
                    )
                else:
                    low = now[j + 1, i, pl.ds(8 * g - 1, 8), :]
                if g == groups - 1:
                    high = jnp.where(
                        row_number == 7, jnp.broadcast_to(halo(0, j), (8, lanes)), pltpu.roll(middle, 7, 0)
                    )
                else:
                    high = now[j + 1, i, pl.ds(8 * g + 1, 8), :]
                spread = (
                    (column[j] + column[j + 2])
                    + (now[j + 1, i - 1, k, :] + now[j + 1, i + 1, k, :])
                    + (low + high)
                    - 6.0 * middle
                )
                later = 2.0 * middle - old[j + 1, i, k, :] + speed[j, i - 1, k, :] * spread
                old[j + 1, i, k, :] = later
                if last:
                    sums[j] = later if g == 0 else sums[j] + later
                else:
                    if g == 0:
                        keep(0, j, later[0:1])
                    if g == groups - 1:
                        keep(1, j, later[7:8])
        if last:
            for j in js:
                total = jnp.sum(sums[j], axis=0, keepdims=True)
                mean = jnp.broadcast_to(total * (1.0 / nk), (8, lanes))
                squares = None
                for g in range(groups):
                    moved = old[j + 1, i, pl.ds(8 * g, 8), :] - mean
                    squares = moved * moved if g == 0 else squares + moved * moved
                square = jnp.sum(squares, axis=0, keepdims=True)
                if rim is None:
                    own_stats[0, 0, j, pl.ds(i - 1, 1), :] = total
                    own_stats[0, 1, j, pl.ds(i - 1, 1), :] = square
                else:
                    own_edge[0, pl.ds(rim * nj + j, 1), :] = total
                    own_edge[1, pl.ds(rim * nj + j, 1), :] = square

    every_j, begun, done = tuple(range(nj)), set(), {}

    def loaded(part):
        if ("load", part) not in begun:
            begun.add(("load", part))
            load("old", part).wait()
            load("speed", part).wait()

    def interior(step, part):
        start, stop = span(part)
        rim = max(step, 1)
        start, stop = max(1 + start, 1 + rim), min(1 + stop, 1 + ni - rim)
        if step == 1:
            loaded(part)
        rows(step - 1, part, "taken")
        slabs(step - 1, part, "taken")
        if step >= 2 and step not in begun:
            begun.add(step)
            rows_sent(step - 2)

        @pl.loop(start, stop)
        def _(i):
            line(step, i, every_j)

        if step < STEPS:
            rows(step, part, "start")
            slabs(step, part, "start")

    def strips(step):
        if step == 2:
            for number, place in ((parts, 2), (parts + 1, ni - 1)):
                line(step, place, every_j)
                rows(step, number, "start")
                slabs(step, number, "start")
        else:
            for number in (parts, parts + 1):
                rows(step - 1, number, "taken")
                slabs(step - 1, number, "taken")
            for place in (3, ni - 2, 2, ni - 1):
                line(step, place, every_j)

    def edge(step, which, j):
        side(step - 1, which, j, "taken")
        pair = (step, which, j // group)
        done[pair] = done.get(pair, 0) + 1
        if done[pair] == 1:
            slab_rim(step - 1, which, j // group, "taken")
        shared = [to_high for to_high, place in ((0, 0), (1, nj - 1)) if place == j]
        row_rim(step - 1, which, [1 - to_high for to_high in shared], "taken")
        if step >= 2 and (step, which) not in begun:
            begun.add((step, which))
            side_sent(step - 2, which)
        if step == 1:
            loaded(0)
            loaded(parts - 1)
        line(step, places[which], (j,), which)
        if half and (step, which, j) == (1, OWN, 0):
            for other in range(half, nj):
                side(0, DIAG, other, "start")
        if step < STEPS:
            side(step, which, j, "start")
            if done[pair] == group:
                slab_rim(step, which, j // group, "start")
            row_rim(step, which, shared, "start")

    levels = n_slabs.bit_length() - 1
    stat_recv = (load_x, load_y, load_c)
    partners = []
    for level in range(levels):
        bit = lax.rem(here["slabs"] // 2**level, 2)
        partners.append(here["slabs"] + (1 - 2 * bit) * 2**level)

    def stat_copy(part, level):
        lines = pl.ds(part * width, width)
        return remote(
            own_stats.at[level, :, :, lines], in_stats.at[level, :, :, lines],
            stat_send, stat_recv[level].at[part], "slabs", partners[level],
        )

    def merged(part, level):
        lines = pl.ds(part * width, width)
        stat_copy(part, level).wait_recv()
        mine, theirs = own_stats[level, :, :, lines, :], in_stats[level, :, :, lines, :]
        cells = float(nk * 2**level)
        apart = (theirs[0] - mine[0]) * (1.0 / cells)
        return mine[0] + theirs[0], mine[1] + theirs[1] + (0.5 * cells) * apart * apart

    def advance(part, level):
        lines = pl.ds(part * width, width)
        total, square = merged(part, level)
        own_stats[level + 1, 0, :, lines, :] = total
        own_stats[level + 1, 1, :, lines, :] = square
        stat_copy(part, level + 1).start()

    whole = float(nk * n_slabs)

    def rescale(part):
        lines = pl.ds(part * width, width)
        total, square = merged(part, levels - 1)
        means[:, lines, :] = total * (1.0 / whole)
        scales[:, lines, :] = lax.rsqrt(square * (1.0 / whole) + EPS)
        start, stop = span(part)

        @pl.loop(max(start, 1), min(stop, ni - 1))
        def _(i):
            for j in range(nj):
                mean = jnp.broadcast_to(means[j, pl.ds(i, 1), :], (8, lanes))
                scale = jnp.broadcast_to(scales[j, pl.ds(i, 1), :], (8, lanes))
                for g in range(groups):
                    k = pl.ds(8 * g, 8)
                    scaled[j, i, k, :] = (field[j + 1, i + 1, k, :] - mean) * scale

    def do(kind, *what):
        if kind == "in":
            interior(what[0], what[1])
        elif kind == "own":
            edge(what[0], OWN, what[1])
        elif kind == "diag":
            edge(what[0], DIAG, what[1])
        elif kind == "pass":
            hand_on(*what)
        elif kind == "strips":
            strips(what[0])
        elif kind == "stats":
            stat_copy(what[0], 0).start()
        elif kind == "advance":
            for level in range(levels - 1):
                advance(what[0], level)
        elif kind == "rescale":
            rescale(what[0])

    for what in agenda(nj, half, parts, inside_out, outside_in):
        do(*what)

    gaps = range(1, n_slabs)
    for gap in gaps:
        remote(own_edge, all_edge.at[gap - 1], edge_send, edge_recv, "slabs", peers[gap - 1]).start()
    for part in outside_in:
        rescale(part)

    for step in range(STEPS):
        if step == 2:
            for which in (OWN, DIAG):
                side_sent(step, which)
            rows_sent(step)
    slabs_sent()
    if half:
        pl.when(relays)(remote(relayed, relayed, pass_send, side_recv.at[0, DIAG, 0], "cols", beside[OWN]).wait_send)
    remote(own_stats, in_stats, stat_send, stat_recv[0].at[0], "slabs", partners[0]).wait_send()
    edges = remote(all_edge, all_edge, edge_send, edge_recv, "slabs", peers[0])
    edges.wait_recv()
    edges.wait_send()


def agenda(nj, half, parts, first, last):
    timed = []

    def spread(times, entries):
        for n, entry in enumerate(entries):
            spot = min(max((n + 0.5) / len(entries) * len(times) - 0.5, 0), len(times) - 1)
            low = int(spot)
            high = min(low + 1, len(times) - 1)
            timed.append((times[low] + (spot - low) * (times[high] - times[low]), len(timed), entry))

    own = {step: [("own", step, n) for n in range(nj)] for step in range(1, STEPS + 1)}
    diag = {step: [("diag", step, n) for n in range(nj)] for step in range(1, STEPS + 1)}
    passes = [[("pass", step, j) for j in range(half)] for step in range(STEPS)]
    spread(FILL[0], [("in", 1, part) for part in first])
    spread(FILL[1], [("in", 2, part) for part in first])
    spread(FILL[2], [("in", 3, part) for part in first])
    for step in range(STEPS):
        spread(PASS[step], passes[step])
        spread(EDGE[step][OWN], own[step + 1])
        spread(EDGE[step][DIAG], diag[step + 1])
    spread([STRIPS[0]], [("strips", 2)])
    spread([STRIPS[1]], [("strips", 3)])
    for n, part in enumerate(last):
        rim = part in (0, parts - 1)
        spread([STATS[rim] + 0.01 * n], [("stats", part)])
        spread([ADVANCE[rim] + 0.01 * n], [("advance", part)])
    return [entry for _, _, entry in sorted(timed, key=lambda spot: spot[:2])]


def finish_kernel(field, scaled, own_edge, all_edge, scaled_hbm, field_hbm, rims, field_sem, scaled_sem):
    nj, ni, nk, lanes = scaled_hbm.shape
    inner = pl.ds(1, ni - 2)
    for j in range(nj):
        pltpu.make_async_copy(field.at[j + 1, pl.ds(1, ni)], field_hbm.at[j], field_sem).start()
        pltpu.make_async_copy(scaled.at[j, inner], scaled_hbm.at[j, inner], scaled_sem).start()
    pieces = [own_edge[...], *(all_edge[gap] for gap in range(all_edge.shape[0]))]
    whole = float(nk * len(pieces))
    means = pieces[0][0]
    for piece in pieces[1:]:
        means = means + piece[0]
    means = means * (1.0 / whole)
    square = None
    for piece in pieces:
        apart = piece[0] * (1.0 / nk) - means
        term = piece[1] + nk * apart * apart
        square = term if square is None else square + term
    scales = lax.rsqrt(square * (1.0 / whole) + EPS)
    places = edge_places(lax.axis_index("cols"), ni)
    for which in (OWN, DIAG):
        for j in range(nj):
            row = which * nj + j
            mean = jnp.broadcast_to(means[row:row + 1], (8, lanes))
            scale = jnp.broadcast_to(scales[row:row + 1], (8, lanes))
            for g in range(nk // 8):
                k = pl.ds(8 * g, 8)
                rims[which, j, k, :] = (field[j + 1, places[which], k, :] - mean) * scale
        pltpu.make_async_copy(rims.at[which], scaled_hbm.at[:, places[which] - 1], scaled_sem).start()
    pltpu.make_async_copy(scaled, scaled_hbm, scaled_sem).wait()
    pltpu.make_async_copy(field.at[pl.ds(1, nj), pl.ds(1, ni)], field_hbm, field_sem).wait()


def shards(counts, relay, field_now, earlier, speed_square):
    nj, ni, nk, lanes = field_now.shape
    n_slabs = counts["slabs"]
    levels = n_slabs.bit_length() - 1
    assert n_slabs == 2**levels and 1 <= levels <= 3
    relay = relay and nj > 1
    parts = line_parts(ni)
    f32 = jnp.float32
    padded = (nj + 2, ni + 2, nk, lanes)
    hbm = pl.BlockSpec(memory_space=pltpu.HBM)
    vmem = pl.BlockSpec(memory_space=pltpu.VMEM)
    cells = nj * ni * nk * lanes
    dma = pltpu.SemaphoreType.DMA
    field, scaled, own_edge, all_edge = pl.pallas_call(
        functools.partial(march_kernel, counts, relay),
        name="march",
        out_shape=(
            pltpu.VMEM(padded, f32),
            pltpu.VMEM((nj, ni, nk, lanes), f32),
            pltpu.VMEM((2, 2 * nj, lanes), f32),
            pltpu.VMEM((n_slabs - 1, 2, 2 * nj, lanes), f32),
        ),
        in_specs=[hbm] * 3,
        out_specs=(vmem,) * 4,
        scratch_shapes=[
            pltpu.VMEM(padded, f32),
            pltpu.VMEM((STEPS, 2, ni, nj, lanes), f32),
            pltpu.VMEM((STEPS, 2, ni, nj, lanes), f32),
            pltpu.VMEM((STEPS, 2, 2, nj, 1, lanes), f32),
            pltpu.VMEM((STEPS, 2, 2, nj, 1, lanes), f32),
            pltpu.VMEM((levels, 2, nj, ni, lanes), f32),
            pltpu.VMEM((levels, 2, nj, ni, lanes), f32),
            pltpu.VMEM((STEPS, max(nj // 2, 1), nk, lanes), f32),
            pltpu.VMEM((nj, ni, lanes), f32),
            pltpu.VMEM((nj, ni, lanes), f32),
            dma(()),
            dma((parts,)),
            dma((parts,)),
            dma((max(parts, 4),)),
            dma((2, 2)),
            dma((2, 2, nj)),
            dma(()),
            dma((2, 2)),
            dma((2 * parts,)),
            dma((2, 2, 2)),
            dma((2,)),
            dma((2 * parts,)),
            dma((2, 2, nj // (2 if nj % 2 == 0 else 1))),
            dma(()),
            dma(()),
            dma(()),
        ],
        compiler_params=pltpu.CompilerParams(
            collective_id=0, has_side_effects=True, vmem_limit_bytes=40 * 2**20
        ),
        cost_estimate=pl.CostEstimate(flops=33 * cells, bytes_accessed=12 * cells, transcendentals=0),
    )(field_now, earlier, speed_square)
    return pl.pallas_call(
        finish_kernel,
        name="finish",
        out_shape=(jax.ShapeDtypeStruct(field_now.shape, f32),) * 2,
        in_specs=[vmem] * 4,
        out_specs=(hbm,) * 2,
        scratch_shapes=[
            pltpu.VMEM((2, nj, nk, lanes), f32),
            dma(()),
            dma(()),
        ],
        compiler_params=pltpu.CompilerParams(vmem_limit_bytes=16 * 2**20),
        cost_estimate=pl.CostEstimate(flops=2 * cells, bytes_accessed=8 * cells, transcendentals=0),
    )(field, scaled, own_edge, all_edge)


def crosses(mesh):
    order = ("rows", "cols", "slabs")
    devices = mesh.devices.transpose([mesh.axis_names.index(axis) for axis in order])
    if devices.shape[1] != 4:
        return False
    one, other = (getattr(devices[0, place, 0], "coords", None) for place in (1, 2))
    return one is not None and sum(a != b for a, b in zip(one, other)) > 1


def solution(mesh):
    spec = P("rows", "cols", "slabs", None)
    return jax.shard_map(
        functools.partial(shards, dict(mesh.shape), crosses(mesh)),
        mesh=mesh,
        in_specs=(spec,) * 3,
        out_specs=(spec,) * 2,
        check_vma=False,
    )
```
